32 devices in a mesh: dp: 1 (over z), tp2: 4 (over y), tp: 8 (over x, core).
Axes of the slice: x: 4, y: 4, z: 1, core: 2. Of those that a mesh axis runs over, the one named last changes fastest.
The devices are a block of a 4x4x8 slice.
Arguments:
- attn_out: bfloat16 [8192, 12288], P('dp', 'tp')
- w_out: bfloat16 [12288, 12288], P('tp', 'tp2')
- residual: bfloat16 [8192, 12288], P(('dp', 'tp'), 'tp2')
- norm_gain: float32 [12288], P('tp2')
Outputs:
- output 1: bfloat16 [8192, 12288], P(('dp', 'tp'), 'tp2')
- output 2: bfloat16 [8192, 12288], P(('dp', 'tp'), 'tp2')
All inputs are finite; a program needn't handle non-finite values.
Results may differ from the reference program's by a relative error of at most 0.00707124.
Values are sent between devices in bfloat16 or wider.
A program may use at most 768 MiB of HBM per device.

```python
import jax
import jax.numpy as jnp
from jax import lax

TOKENS = 8192
D = 12288
HEADS = 96
HEAD = 128
TP = 8
EPS_NORM = 1e-6


def setup_inputs(seed: int = 0, part: int = 0) -> dict:
    attn_width = HEADS * HEAD
    root_key = jax.random.key(seed)
    key_attn, key_w, key_res, key_gain = jax.random.split(root_key, 4)
    attn_vals = jax.random.normal(jax.random.fold_in(key_attn, part), (TOKENS, attn_width), jnp.float32)
    w_vals = jax.random.normal(key_w, (attn_width, D), jnp.float32) * (attn_width ** -0.5)
    res_vals = jax.random.normal(jax.random.fold_in(key_res, part), (TOKENS, D), jnp.float32)
    gain_vals = 1.0 + 0.3 * jax.random.normal(key_gain, (D,), jnp.float32)
    return {"attn_out": attn_vals.astype(jnp.bfloat16), "w_out": w_vals.astype(jnp.bfloat16), "residual": res_vals.astype(jnp.bfloat16), "norm_gain": gain_vals}


def reference(attn_out, w_out, residual, norm_gain):
    attn_width = attn_out.shape[1]
    shard_cols = attn_width // TP
    attn_shards = attn_out.reshape(TOKENS, TP, shard_cols).transpose(1, 0, 2)
    w_shards = w_out.reshape(TP, shard_cols, D)

    def add_shard(running, shard_pair):
        attn_blk, w_blk = shard_pair
        block_prod = jnp.dot(attn_blk, w_blk, preferred_element_type=jnp.float32).astype(jnp.bfloat16)
        return running + block_prod.astype(jnp.float32), None

    y_sum, _ = lax.scan(add_shard, jnp.zeros((TOKENS, D), jnp.float32), (attn_shards, w_shards))
    hidden = residual.astype(jnp.float32) + y_sum
    mean_sq = jnp.mean(hidden * hidden, axis=-1, keepdims=True)
    normed = hidden * lax.rsqrt(mean_sq + EPS_NORM) * norm_gain
    return hidden.astype(jnp.bfloat16), normed.astype(jnp.bfloat16)
```

```python
import functools

import jax
import jax.numpy as jnp
from jax import lax
from jax.experimental import pallas as pl
from jax.experimental.pallas import tpu as pltpu
from jax.sharding import PartitionSpec as P

EPS_NORM = 1e-6
MESH = pl.DeviceIdType.MESH
CORES = 2
CN = 256
WS = 3
LAG = 2
AHEAD = 3


def kernel(ny, chips, a, w, r, h_out, ssq_out, wbuf, av, wv, ov, rbuf, lv, rv, hv, ssacc, svr,
           al_sem, ap_send, ap_recv, ax_send, ax_recv, ay_send, ay_recv, af_send, af_recv,
           wp_send, wp_recv, wa_send, wa_recv, wf_send, wf_recv, o_send, o_recv,
           wl_sem, r_sem, h_sem, s_send, s_recv):
    rows, cols = r.shape
    chunks = cols // CN
    quarter = rows // ny
    tile = min(256, rows)
    me, y = lax.axis_index("tp"), lax.axis_index("tp2")
    x, c = lax.div(me, CORES), lax.rem(me, CORES)
    o = 1 - c
    xa = x + 1 - 2 * lax.rem(x, 2)
    xb = chips - 1 - x
    xab = chips - 1 - xa
    yp, ym = lax.rem(y + 1, ny), lax.rem(y + ny - 1, ny)
    part = {"tp": x * CORES + o}
    acore, aother = {"tp": xa * CORES + c}, {"tp": xa * CORES + o}
    bcore = {"tp": xb * CORES + c}
    up, down = {"tp2": yp}, {"tp2": ym}

    def remote(src, dst, send, recv, device):
        return pltpu.make_async_remote_copy(
            src_ref=src, dst_ref=dst, send_sem=send, recv_sem=recv, device_id=device, device_id_type=MESH)

    def arow(owner, size=None, shift=0):
        return pl.ds(pl.multiple_of(owner * rows + shift, 16), rows if size is None else size)

    def qrow(q):
        return pl.ds(pl.multiple_of(q * quarter, 16), quarter)

    def wcol(j):
        return pl.ds(pl.multiple_of(j * CN, CN), CN)

    own_rows = (xb * CORES + c, me)
    part_rows = (xb * CORES + o, x * CORES + o)

    def a_local(g):
        return pltpu.make_async_copy(a.at[arow(own_rows[g])], av.at[g, 0], al_sem.at[g])

    def a_part(g):
        return remote(a.at[arow(part_rows[g])], av.at[g, 1], ap_send.at[g], ap_recv.at[g], part)

    def a_cross(g, s):
        core, device = ((c, acore), (o, aother))[s]
        owner = (xab, xa)[g] * CORES + core
        return remote(a.at[arow(owner, quarter, y * quarter)], av.at[g, 2 + s, qrow(y)],
                      ax_send.at[g, s], ax_recv.at[g, s], device)

    def a_near(g, s, d):
        ref = av.at[g, 2 + s, qrow(y)]
        return remote(ref, ref, ay_send.at[g, s, d], ay_recv.at[g, s, d], (up, down)[d])

    def a_far(g, s):
        ref = av.at[g, 2 + s, qrow((ym, yp)[s])]
        return remote(ref, ref, af_send.at[g, s], af_recv.at[g, s], (up, down)[s])

    def a_first(g):
        for s in range(2):
            a_cross(g, s).wait_recv()
            for d in range(2):
                a_near(g, s, d).start()

    def a_second(g):
        for s in range(2):
            a_near(g, s, s).wait_recv()
            a_far(g, s).start()

    def a_third(g):
        a_local(g).wait()
        a_part(g).wait_recv()
        for s in range(2):
            a_near(g, s, 1 - s).wait_recv()
            a_far(g, s).wait_recv()

    def w_part(j):
        return remote(w.at[:, wcol(j)], wbuf.at[0, j], wp_send.at[j], wp_recv.at[j], part)

    def w_cross(j):
        return remote(w.at[:, wcol(j)], wbuf.at[1, j], wa_send.at[j], wa_recv.at[j], acore)

    def w_pass(j):
        return remote(wbuf.at[1, j], wbuf.at[2, j], wf_send.at[j], wf_recv.at[j], part)

    def w_load(j, k):
        src = w.at[:, wcol(j)] if k == 0 else wbuf.at[k - 1, j]
        return pltpu.make_async_copy(src, wv.at[lax.rem(j, WS), k], wl_sem.at[k])

    def out_copy(j):
        slot = lax.rem(j, 2)
        return remote(ov.at[slot], rbuf.at[j], o_send.at[slot], o_recv.at[j], bcore)

    def r_load(j):
        return pltpu.make_async_copy(r.at[:, wcol(j)], rv, r_sem)

    def h_store(j):
        slot = lax.rem(j, 2)
        return pltpu.make_async_copy(hv.at[slot], h_out.at[:, wcol(j)], h_sem.at[slot])

    def gemm(g, j, dst):
        slot = lax.rem(j, WS)

        def step(i, carry):
            rs = pl.ds(pl.multiple_of(i * tile, tile), tile)
            acc = None
            for k in range(4):
                prod = jnp.dot(av[g, k, rs, :], wv[slot, k], preferred_element_type=jnp.float32)
                prod = prod.astype(jnp.bfloat16).astype(jnp.float32)
                acc = prod if acc is None else acc + prod
            dst[rs, :] = acc
            return carry

        lax.fori_loop(0, rows // tile, step, 0)

    barrier = pltpu.get_barrier_semaphore()
    peers = [part, acore, aother, bcore] + [{"tp2": lax.rem(y + d, ny)} for d in range(1, ny)]
    for peer in peers:
        pl.semaphore_signal(barrier, inc=1, device_id=peer, device_id_type=MESH)
    pl.semaphore_wait(barrier, len(peers))

    for s in range(2):
        a_cross(0, s).start()
    a_part(0).start()
    w_cross(0).start()
    w_part(0).start()
    w_cross(1).start()
    w_part(1).start()
    for s in range(2):
        a_cross(1, s).start()
    a_part(1).start()
    for j in range(2, AHEAD):
        w_cross(j).start()
        w_part(j).start()
    a_local(0).start()
    a_local(1).start()
    ssacc[...] = jnp.zeros_like(ssacc)
    a_first(0)
    a_second(0)
    a_third(0)

    def step(j, carry):
        @pl.when(j < chunks)
        def _():
            w_cross(j).wait_recv()
            w_pass(j).start()

            @pl.when(j + AHEAD < chunks)
            def _():
                w_cross(j + AHEAD).start()
                w_part(j + AHEAD).start()

            w_load(j, 0).start()
            w_load(j, 2).start()
            w_part(j).wait_recv()
            w_load(j, 1).start()
            w_pass(j).wait_recv()
            w_load(j, 3).start()

            @pl.when(j >= 2)
            def _():
                out_copy(j - 2).wait_send()

            for k in range(4):
                w_load(j, k).wait()
            gemm(0, j, ov.at[lax.rem(j, 2)])

        @pl.when(j == 1)
        def _():
            a_first(1)

        @pl.when(j == 2)
        def _():
            a_second(1)
            a_third(1)

        @pl.when(j >= LAG)
        def _():
            r_load(j - LAG).start()

        @pl.when(j < chunks)
        def _():
            out_copy(j).start()

        @pl.when(j >= LAG)
        def _():
            i = j - LAG
            gemm(1, i, lv)
            r_load(i).wait()
            slot = lax.rem(i, 2)

            @pl.when(i >= 2)
            def _():
                h_store(i - 2).wait()

            out_copy(i).wait_recv()

            def merge(t, carry):
                rs = pl.ds(pl.multiple_of(t * 64, 64), 64)
                h = rv[rs, :].astype(jnp.float32) + (lv[rs, :] + rbuf[i, rs, :])
                hv[slot, rs, :] = h
                sq = h * h
                acc = ssacc[rs, :]
                for l in range(CN // 128):
                    acc = acc + sq[:, l * 128:(l + 1) * 128]
                ssacc[rs, :] = acc
                return carry

            lax.fori_loop(0, rows // 64, merge, 0)
            h_store(i).start()

        return carry

    lax.fori_loop(0, chunks + LAG, step, 0)

    svr[y] = lax.dot_general(jnp.ones((8, 128), jnp.float32), ssacc[...], (((1,), (1,)), ((), ())),
                             preferred_element_type=jnp.float32, precision=lax.Precision.HIGHEST)
    h_store(chunks - 2).wait()
    h_store(chunks - 1).wait()
    sums = [remote(svr.at[y], svr.at[y], s_send.at[d - 1], s_recv.at[d - 1], {"tp2": lax.rem(y + d, ny)})
            for d in range(1, ny)]
    for copy in sums:
        copy.start()

    def drain(j, carry):
        w_cross(j).wait_send()
        w_part(j).wait_send()
        w_pass(j).wait_send()
        return carry

    lax.fori_loop(0, chunks, drain, 0)
    for g in range(2):
        a_part(g).wait_send()
        for s in range(2):
            a_cross(g, s).wait_send()
            a_far(g, s).wait_send()
            for d in range(2):
                a_near(g, s, d).wait_send()
    out_copy(chunks - 2).wait_send()
    out_copy(chunks - 1).wait_send()
    for d in range(1, ny):
        src = lax.rem(y + ny - d, ny)
        remote(svr.at[src], svr.at[src], s_send.at[d - 1], s_recv.at[d - 1], part).wait_recv()
    total = svr[0]
    for q in range(1, ny):
        total = total + svr[q]
    ssq_out[...] = total
    for copy in sums:
        copy.wait_send()


def solution(mesh):
    tp, ny = mesh.shape["tp"], mesh.shape["tp2"]
    chips = tp // CORES

    def local_step(a, w, r, gain):
        depth, cols = w.shape
        rows = r.shape[0]
        chunks = cols // CN
        dma = pltpu.SemaphoreType.DMA
        any_space = pl.BlockSpec(memory_space=pl.ANY)
        hidden, ssq, _ = pl.pallas_call(
            functools.partial(kernel, ny, chips),
            out_shape=(
                jax.ShapeDtypeStruct((rows, cols), jnp.float32),
                jax.ShapeDtypeStruct((8, rows), jnp.float32),
                jax.ShapeDtypeStruct((3, chunks, depth, CN), jnp.bfloat16),
            ),
            in_specs=[any_space] * 3,
            out_specs=(any_space, pl.BlockSpec(memory_space=pltpu.VMEM), any_space),
            scratch_shapes=[
                pltpu.VMEM((2, 4, rows, depth), jnp.bfloat16),
                pltpu.VMEM((WS, 4, depth, CN), jnp.bfloat16),
                pltpu.VMEM((2, rows, CN), jnp.float32),
                pltpu.VMEM((chunks, rows, CN), jnp.float32),
                pltpu.VMEM((rows, CN), jnp.float32),
                pltpu.VMEM((rows, CN), jnp.bfloat16),
                pltpu.VMEM((2, rows, CN), jnp.float32),
                pltpu.VMEM((rows, 128), jnp.float32),
                pltpu.VMEM((ny, 8, rows), jnp.float32),
                dma((2,)), dma((2,)), dma((2,)), dma((2, 2)), dma((2, 2)),
                dma((2, 2, 2)), dma((2, 2, 2)), dma((2, 2)), dma((2, 2)),
                dma((chunks,)), dma((chunks,)), dma((chunks,)), dma((chunks,)), dma((chunks,)), dma((chunks,)),
                dma((2,)), dma((chunks,)),
                dma((4,)), dma(()), dma((2,)), dma((ny - 1,)), dma((ny - 1,)),
            ],
            compiler_params=pltpu.CompilerParams(
                collective_id=0, has_side_effects=True, vmem_limit_bytes=67043328),
            cost_estimate=pl.CostEstimate(
                flops=2 * 8 * rows * depth * cols, bytes_accessed=8 * depth * cols * 2, transcendentals=0),
        )(a, w, r)
        inv_rms = lax.rsqrt(ssq[0] / (cols * ny) + EPS_NORM)
        normed = hidden * inv_rms[:, None] * gain
        return hidden.astype(jnp.bfloat16), normed.astype(jnp.bfloat16)

    row_spec = P(("dp", "tp"), "tp2")
    return jax.shard_map(local_step, mesh=mesh, in_specs=(P("dp", "tp"), P("tp", "tp2"), row_spec, P("tp2")),
                         out_specs=(row_spec, row_spec), check_vma=False)
```

```python
import functools

import jax
import jax.numpy as jnp
from jax import lax
from jax.experimental import pallas as pl
from jax.experimental.pallas import tpu as pltpu
from jax.sharding import PartitionSpec as P

EPS_NORM = 1e-6
MESH = pl.DeviceIdType.MESH
CORES = 2
CN = 256
LAG = 6
AHEAD = 6
PIECES = 4


def kernel(ny, chips, a, w, r, h_out, ssq_out, wbuf, av, wv, ov, rbuf, lv, rv, hv, ssacc, svr,
           at, pv, sb, sp, sf, sg,
           al_sem, ap_send, ap_recv, ax_send, ax_recv, ay_send, ay_recv, af_send, af_recv,
           wp_send, wp_recv, wa_send, wa_recv, wf_send, wf_recv, o_send, o_recv,
           wl_sem, r_sem, h_sem, s_send, s_recv, at_sem, sb_send, sb_recv, sp_send, sp_recv, sf_send, sf_recv):
    rows, cols = r.shape
    last = cols // CN - 1
    quarter = rows // ny
    piece = quarter // PIECES
    tile = min(256, rows)
    me, y = lax.axis_index("tp"), lax.axis_index("tp2")
    x, c = lax.div(me, CORES), lax.rem(me, CORES)
    o = 1 - c
    xa = x + 1 - 2 * lax.rem(x, 2)
    xb = chips - 1 - x
    xab = chips - 1 - xa
    yp, ym = lax.rem(y + 1, ny), lax.rem(y + ny - 1, ny)
    part = {"tp": x * CORES + o}
    acore, aother = {"tp": xa * CORES + c}, {"tp": xa * CORES + o}
    bcore, bother = {"tp": xb * CORES + c}, {"tp": xb * CORES + o}
    up, down = {"tp2": yp}, {"tp2": ym}

    def remote(src, dst, send, recv, device):
        return pltpu.make_async_remote_copy(
            src_ref=src, dst_ref=dst, send_sem=send, recv_sem=recv, device_id=device, device_id_type=MESH)

    def arow(owner, size=None, shift=0):
        return pl.ds(pl.multiple_of(owner * rows + shift, 16), rows if size is None else size)

    def qrow(q, t):
        return pl.ds(pl.multiple_of(q * quarter + t * piece, 16), piece)

    def wcol(j):
        return pl.ds(pl.multiple_of(j * CN, CN), CN)

    own_rows = (xb * CORES + c, me)
    part_rows = (xb * CORES + o, x * CORES + o)

    def a_local(g):
        return pltpu.make_async_copy(a.at[arow(own_rows[g])], av.at[g, 0], al_sem.at[g])

    def a_part(g):
        return remote(a.at[arow(part_rows[g])], av.at[g, 1], ap_send.at[g], ap_recv.at[g], part)

    def a_cross(g, s, t):
        core, device = ((c, acore), (o, aother))[s]
        owner = (xab, xa)[g] * CORES + core
        return remote(a.at[arow(owner, piece, y * quarter + t * piece)], av.at[g, 2 + s, qrow(y, t)],
                      ax_send.at[g, s, t], ax_recv.at[g, s, t], device)

    def a_near(g, s, t, d):
        ref = av.at[g, 2 + s, qrow(y, t)]
        return remote(ref, ref, ay_send.at[g, s, t, d], ay_recv.at[g, s, t, d], (up, down)[d])

    def a_far(g, s, t):
        ref = av.at[g, 2 + s, qrow((ym, yp)[s], t)]
        return remote(ref, ref, af_send.at[g, s, t], af_recv.at[g, s, t], (up, down)[s])

    def a_send(g, s):
        for t in range(PIECES):
            a_cross(g, s, t).start()

    def a_first(g, s, t):
        a_cross(g, s, t).wait_recv()
        for d in range(2):
            a_near(g, s, t, d).start()

    def a_second(g, s, t):
        a_near(g, s, t, s).wait_recv()
        a_far(g, s, t).start()

    def a_third(g):
        a_local(g).wait()
        a_part(g).wait_recv()
        for t in range(PIECES):
            for s in range(2):
                a_near(g, s, t, 1 - s).wait_recv()
                a_far(g, s, t).wait_recv()

    def w_part(j):
        return remote(w.at[:, wcol(j)], wbuf.at[0, j], wp_send.at[j], wp_recv.at[j], part)

    def w_cross(j):
        return remote(w.at[:, wcol(j)], wbuf.at[1, j], wa_send.at[j], wa_recv.at[j], acore)

    def w_pass(j):
        return remote(wbuf.at[1, j], wbuf.at[2, j], wf_send.at[j], wf_recv.at[j], part)

    def w_load(g, j, k):
        src = w.at[:, wcol(j)] if k == 0 else wbuf.at[k - 1, j]
        return pltpu.make_async_copy(src, wv.at[g, k], wl_sem.at[g, k])

    def out_copy(j):
        slot = lax.rem(j, 2)
        return remote(ov.at[slot], rbuf.at[j], o_send.at[slot], o_recv.at[j], bcore)

    def r_load(j):
        return pltpu.make_async_copy(r.at[:, wcol(j)], rv, r_sem)

    def h_store(j):
        return pltpu.make_async_copy(hv, h_out.at[:, wcol(j)], h_sem)

    def block_product(lhs, rhs):
        return jnp.dot(lhs, rhs, preferred_element_type=jnp.float32).astype(jnp.bfloat16)

    def gemm(g, dst):
        def step(i, carry):
            rs = pl.ds(pl.multiple_of(i * tile, tile), tile)
            acc = None
            for k in range(4):
                prod = block_product(av[g, k, rs, :], wv[g, k]).astype(jnp.float32)
                acc = prod if acc is None else acc + prod
            dst[rs, :] = acc
            return carry

        lax.fori_loop(0, rows // tile, step, 0)

    items = ((xb, 0), (xb, 1), (xab, 0), (xab, 1), (x, o), (xa, o), (x, c), (xa, c))

    def at_load(n):
        pos, core = items[n]
        return pltpu.make_async_copy(a.at[arow(pos * CORES + core)], at.at[n % 2], at_sem.at[n % 2])

    def item_send(n):
        if n < 4:
            slot = n // 2 * 2 + c
            device = {"tp": xb * CORES + n % 2}
            return remote(pv.at[n], sb.at[slot], sb_send.at[n], sb_recv.at[slot], device)
        return remote(pv.at[n], sp.at[n - 4], sp_send.at[n - 4], sp_recv.at[n - 4], part)

    def item(n):
        at_load(n).wait()

        def step(i, carry):
            rs = pl.ds(pl.multiple_of(i * tile, tile), tile)
            pv[n, rs, :] = block_product(at[n % 2, rs, :], wv[0, 0])
            return carry

        lax.fori_loop(0, rows // tile, step, 0)
        if n + 2 < len(items):
            at_load(n + 2).start()

    def sb_arrival(slot):
        return remote(pv.at[0], sb.at[slot], sb_send.at[0], sb_recv.at[slot], bcore)

    def sf_copy():
        return remote(sg, sf, sf_send, sf_recv, acore)

    def for_rows(body):
        def step(t, carry):
            body(pl.ds(pl.multiple_of(t * 64, 64), 64))
            return carry

        lax.fori_loop(0, rows // 64, step, 0)

    def finish(rs, h):
        hv[rs, :] = h
        sq = h * h
        acc = ssacc[rs, :]
        for l in range(CN // 128):
            acc = acc + sq[:, l * 128:(l + 1) * 128]
        ssacc[rs, :] = acc

    def wide(v):
        return v.astype(jnp.float32)

    barrier = pltpu.get_barrier_semaphore()
    peers = [part, acore, aother, bcore, bother] + [{"tp2": lax.rem(y + d, ny)} for d in range(1, ny)]
    for peer in peers:
        pl.semaphore_signal(barrier, inc=1, device_id=peer, device_id_type=MESH)
    w_last = pltpu.make_async_copy(w.at[:, wcol(last)], wv.at[0, 0], wl_sem.at[0, 0])
    w_last.start()
    at_load(0).start()
    at_load(1).start()
    pl.semaphore_wait(barrier, len(peers))

    for t in range(PIECES):
        for s in range(2):
            a_cross(0, s, t).start()
    a_part(0).start()
    for j in range(AHEAD):
        w_cross(j).start()
        w_part(j).start()
        if j == 3:
            a_send(1, 0)
        if j == 4:
            a_send(1, 1)
    a_part(1).start()
    w_last.wait()
    with jax.named_scope("items"):
        item(0)
        item(1)
        item_send(0).start()
        item(2)
        item_send(1).start()
        item(3)
        item_send(2).start()
    a_local(0).start()
    a_local(1).start()
    ssacc[...] = jnp.zeros_like(ssacc)
    item_send(3).start()
    with jax.named_scope("a0_first"):
        for t in range(PIECES):
            for s in range(2):
                a_first(0, s, t)
    with jax.named_scope("items_2"):
        for n in range(4, 8):
            item(n)
        item_send(4).start()
        item_send(5).start()
    with jax.named_scope("a0_second"):
        for t in range(PIECES):
            for s in range(2):
                a_second(0, s, t)
    with jax.named_scope("a0_third"):
        a_third(0)

    def merge_last(before):
        r_load(before + 1).wait()
        h_store(before).wait()
        r_load(last).start()
        sb_arrival(0).wait_recv()
        sb_arrival(1).wait_recv()
        with jax.named_scope("sf_wait"):
            sf_copy().wait_recv()
        r_load(last).wait()
        for_rows(lambda rs: finish(rs, wide(rv[rs, :]) + (
            (wide(pv[6, rs, :]) + wide(sp[0, rs, :])) + (wide(sb[0, rs, :]) + wide(sb[1, rs, :])) + sf[rs, :])))
        h_store(last).start()
        r_load(before + 1).start()

    def sum_last():
        for n in range(2):
            item_send(4 + n).wait_recv()
            sb_arrival(2 + n).wait_recv()

        def body(rs):
            sg[rs, :] = (wide(pv[7, rs, :]) + wide(sp[1, rs, :])) + (wide(sb[2, rs, :]) + wide(sb[3, rs, :]))

        for_rows(body)

    def step(j, carry):
        @pl.when(j < last)
        def _():
            with jax.named_scope("w_cross_wait"):
                w_cross(j).wait_recv()
            w_pass(j).start()

            @pl.when(j + AHEAD < last)
            def _():
                w_cross(j + AHEAD).start()
                w_part(j + AHEAD).start()

            w_load(0, j, 0).start()
            w_load(0, j, 2).start()
            with jax.named_scope("w_pass_wait"):
                w_part(j).wait_recv()
                w_load(0, j, 1).start()
                w_pass(j).wait_recv()
                w_load(0, j, 3).start()

            @pl.when(j >= 2)
            def _():
                with jax.named_scope("o_send_wait"):
                    out_copy(j - 2).wait_send()

            with jax.named_scope("w_load_wait"):
                for k in range(4):
                    w_load(0, j, k).wait()
            with jax.named_scope("gemm0"):
                gemm(0, ov.at[lax.rem(j, 2)])

        @pl.when(j >= LAG)
        def _():
            for k in range(4):
                w_load(1, j - LAG, k).start()
            r_load(j - LAG).start()

        @pl.when(j < last)
        def _():
            out_copy(j).start()

        @pl.when(j == 4)
        def _():
            with jax.named_scope("a1_4"):
                for t in range(PIECES):
                    a_first(1, 0, t)

        @pl.when(j == 5)
        def _():
            with jax.named_scope("a1_5"):
                for t in range(PIECES):
                    a_first(1, 1, t)
                for t in range(PIECES):
                    a_second(1, 0, t)

        @pl.when(j == LAG)
        def _():
            with jax.named_scope("a1_6"):
                for t in range(PIECES):
                    a_second(1, 1, t)
                a_third(1)

        @pl.when(j == last - 3)
        def _():
            with jax.named_scope("sum_last"):
                sum_last()

        @pl.when(j == last + 1)
        def _():
            with jax.named_scope("merge_last"):
                merge_last(j - LAG - 1)

        @pl.when(j >= LAG)
        def _():
            i = j - LAG
            with jax.named_scope("local_load_wait"):
                for k in range(4):
                    w_load(1, i, k).wait()
                r_load(i).wait()
            with jax.named_scope("gemm1"):
                gemm(1, lv)

            @pl.when(i >= 1)
            def _():
                h_store(i - 1).wait()

            with jax.named_scope("o_recv_wait"):
                out_copy(i).wait_recv()
            with jax.named_scope("merge"):
                for_rows(lambda rs: finish(rs, wide(rv[rs, :]) + (lv[rs, :] + rbuf[i, rs, :])))
            h_store(i).start()

        @pl.when(j == last - 3)
        def _():
            sf_copy().start()

        return carry

    lax.fori_loop(0, last + LAG, step, 0)

    svr[y] = lax.dot_general(jnp.ones((8, 128), jnp.float32), ssacc[...], (((1,), (1,)), ((), ())),
                             preferred_element_type=jnp.float32, precision=lax.Precision.HIGHEST)

    def drain(j, carry):
        w_cross(j).wait_send()
        w_part(j).wait_send()
        w_pass(j).wait_send()
        return carry

    lax.fori_loop(0, last, drain, 0)
    for g in range(2):
        a_part(g).wait_send()
        for s in range(2):
            for t in range(PIECES):
                a_cross(g, s, t).wait_send()
                a_far(g, s, t).wait_send()
                for d in range(2):
                    a_near(g, s, t, d).wait_send()
    for n in range(6):
        item_send(n).wait_send()
    sf_copy().wait_send()
    sums = [remote(svr.at[y], svr.at[y], s_send.at[d - 1], s_recv.at[d - 1], {"tp2": lax.rem(y + d, ny)})
            for d in range(1, ny)]
    for copy in sums:
        copy.start()
    out_copy(last - 2).wait_send()
    out_copy(last - 1).wait_send()
    h_store(last - 1).wait()
    for d in range(1, ny):
        src = lax.rem(y + ny - d, ny)
        remote(svr.at[src], svr.at[src], s_send.at[d - 1], s_recv.at[d - 1], part).wait_recv()
    total = svr[0]
    for q in range(1, ny):
        total = total + svr[q]
    ssq_out[...] = total
    for copy in sums:
        copy.wait_send()


def norm_kernel(width, h, ssq, gain, hidden, normed):
    inv_rms = lax.rsqrt(ssq[...] / width + EPS_NORM)
    scale = jnp.transpose(inv_rms)[:, :1]
    value = h[...]
    hidden[...] = value.astype(jnp.bfloat16)
    normed[...] = (value * scale * gain[...]).astype(jnp.bfloat16)


def solution(mesh):
    tp, ny = mesh.shape["tp"], mesh.shape["tp2"]
    chips = tp // CORES

    def local_step(a, w, r, gain):
        depth, cols = w.shape
        rows = r.shape[0]
        last = cols // CN - 1
        dma = pltpu.SemaphoreType.DMA
        any_space = pl.BlockSpec(memory_space=pl.ANY)
        bf16, f32 = jnp.bfloat16, jnp.float32
        h, ssq, _ = pl.pallas_call(
            functools.partial(kernel, ny, chips),
            out_shape=(
                jax.ShapeDtypeStruct((rows, cols), f32),
                jax.ShapeDtypeStruct((8, rows), f32),
                jax.ShapeDtypeStruct((3, last, depth, CN), bf16),
            ),
            in_specs=[any_space] * 3,
            out_specs=(any_space, pl.BlockSpec(memory_space=pltpu.VMEM), any_space),
            scratch_shapes=[
                pltpu.VMEM((2, 4, rows, depth), bf16),
                pltpu.VMEM((2, 4, depth, CN), bf16),
                pltpu.VMEM((2, rows, CN), f32),
                pltpu.VMEM((last, rows, CN), f32),
                pltpu.VMEM((rows, CN), f32),
                pltpu.VMEM((rows, CN), bf16),
                pltpu.VMEM((rows, CN), f32),
                pltpu.VMEM((rows, 128), f32),
                pltpu.VMEM((ny, 8, rows), f32),
                pltpu.VMEM((2, rows, depth), bf16),
                pltpu.VMEM((8, rows, CN), bf16),
                pltpu.VMEM((4, rows, CN), bf16),
                pltpu.VMEM((2, rows, CN), bf16),
                pltpu.VMEM((rows, CN), f32),
                pltpu.VMEM((rows, CN), f32),
                dma((2,)), dma((2,)), dma((2,)), dma((2, 2, PIECES)), dma((2, 2, PIECES)),
                dma((2, 2, PIECES, 2)), dma((2, 2, PIECES, 2)), dma((2, 2, PIECES)), dma((2, 2, PIECES)),
                dma((last,)), dma((last,)), dma((last,)), dma((last,)), dma((last,)), dma((last,)),
                dma((2,)), dma((last,)),
                dma((2, 4)), dma(()), dma(()), dma((ny - 1,)), dma((ny - 1,)),
                dma((2,)), dma((4,)), dma((4,)), dma((2,)), dma((2,)), dma(()), dma(()),
            ],
            compiler_params=pltpu.CompilerParams(
                collective_id=0, has_side_effects=True, vmem_limit_bytes=67043328),
            cost_estimate=pl.CostEstimate(
                flops=2 * 8 * rows * depth * cols, bytes_accessed=8 * depth * cols * 2, transcendentals=0),
        )(a, w, r)
        span = 128
        row_block = pl.BlockSpec((span, cols), lambda i: (i, 0))
        return pl.pallas_call(
            functools.partial(norm_kernel, cols * ny),
            grid=(rows // span,),
            out_shape=(jax.ShapeDtypeStruct((rows, cols), bf16),) * 2,
            in_specs=[row_block, pl.BlockSpec((8, span), lambda i: (0, i)), pl.BlockSpec((1, cols), lambda i: (0, 0))],
            out_specs=(row_block, row_block),
            cost_estimate=pl.CostEstimate(flops=4 * rows * cols, bytes_accessed=8 * rows * cols, transcendentals=rows),
        )(h, ssq, gain.reshape(1, cols))

    row_spec = P(("dp", "tp"), "tp2")
    return jax.shard_map(local_step, mesh=mesh, in_specs=(P("dp", "tp"), P("tp", "tp2"), row_spec, P("tp2")),
                         out_specs=(row_spec, row_spec), check_vma=False)
```

```python
import functools

import jax
import jax.numpy as jnp
from jax import lax
from jax.experimental import pallas as pl
from jax.experimental.pallas import tpu as pltpu
from jax.sharding import PartitionSpec as P

EPS_NORM = 1e-6
MESH = pl.DeviceIdType.MESH
CORES = 2
CN = 256
LAG = 7
AHEAD = 7
PIECES = 4


def kernel(ny, chips, a, w, r, hbuf, ssq_out, wbuf, av, wv, ov, lv, rv, ssacc, svr, at, pv, sb, sp, sg,
           al_sem, ap_send, ap_recv, ax_send, ax_recv, ay_send, ay_recv, af_send, af_recv,
           wp_send, wp_recv, wa_send, wa_recv, wf_send, wf_recv, o_send, o_recv,
           wl_sem, r_sem, s_send, s_recv, at_sem, sb_send, sb_recv, sp_send, sp_recv, sf_send, sf_recv):
    rows, cols = r.shape
    last = cols // CN - 1
    quarter = rows // ny
    piece = quarter // PIECES
    tile = min(256, rows)
    me, y = lax.axis_index("tp"), lax.axis_index("tp2")
    x, c = lax.div(me, CORES), lax.rem(me, CORES)
    o = 1 - c
    xa = x + 1 - 2 * lax.rem(x, 2)
    xb = chips - 1 - x
    xab = chips - 1 - xa
    yp, ym = lax.rem(y + 1, ny), lax.rem(y + ny - 1, ny)
    part = {"tp": x * CORES + o}
    acore, aother = {"tp": xa * CORES + c}, {"tp": xa * CORES + o}
    bcore, bother = {"tp": xb * CORES + c}, {"tp": xb * CORES + o}
    up, down = {"tp2": yp}, {"tp2": ym}

    def remote(src, dst, send, recv, device):
        return pltpu.make_async_remote_copy(
            src_ref=src, dst_ref=dst, send_sem=send, recv_sem=recv, device_id=device, device_id_type=MESH)

    def arow(owner, size=None, shift=0):
        return pl.ds(pl.multiple_of(owner * rows + shift, 16), rows if size is None else size)

    def qrow(q, t):
        return pl.ds(pl.multiple_of(q * quarter + t * piece, 16), piece)

    def wcol(j):
        return pl.ds(pl.multiple_of(j * CN, CN), CN)

    own_rows = (xb * CORES + c, me)
    part_rows = (xb * CORES + o, x * CORES + o)

    def a_local(g):
        return pltpu.make_async_copy(a.at[arow(own_rows[g])], av.at[g, 0], al_sem.at[g])

    def a_part(g):
        return remote(a.at[arow(part_rows[g])], av.at[g, 1], ap_send.at[g], ap_recv.at[g], part)

    def a_cross(g, s, t):
        core, device = ((c, acore), (o, aother))[s]
        owner = (xab, xa)[g] * CORES + core
        return remote(a.at[arow(owner, piece, y * quarter + t * piece)], av.at[g, 2 + s, qrow(y, t)],
                      ax_send.at[g, s, t], ax_recv.at[g, s, t], device)

    def a_near(g, s, t, d):
        ref = av.at[g, 2 + s, qrow(y, t)]
        return remote(ref, ref, ay_send.at[g, s, t, d], ay_recv.at[g, s, t, d], (up, down)[d])

    def a_far(g, s, t):
        ref = av.at[g, 2 + s, qrow((ym, yp)[s], t)]
        return remote(ref, ref, af_send.at[g, s, t], af_recv.at[g, s, t], (up, down)[s])

    def a_send(g, s):
        for t in range(PIECES):
            a_cross(g, s, t).start()

    def a_first(g, s, t):
        a_cross(g, s, t).wait_recv()
        for d in range(2):
            a_near(g, s, t, d).start()

    def a_second(g, s, t):
        a_near(g, s, t, s).wait_recv()
        a_far(g, s, t).start()

    def a_third(g):
        a_local(g).wait()
        a_part(g).wait_recv()
        for t in range(PIECES):
            for s in range(2):
                a_near(g, s, t, 1 - s).wait_recv()

    def a_fourth(g):
        for t in range(PIECES):
            for s in range(2):
                a_far(g, s, t).wait_recv()

    def w_part(j):
        return remote(w.at[:, wcol(j)], wbuf.at[0, j], wp_send.at[j], wp_recv.at[j], part)

    def w_cross(j):
        return remote(w.at[:, wcol(j)], wbuf.at[1, j], wa_send.at[j], wa_recv.at[j], acore)

    def w_pass(j):
        return remote(wbuf.at[1, j], wbuf.at[2, j], wf_send.at[j], wf_recv.at[j], part)

    def w_load(g, j, k):
        src = w.at[:, wcol(j)] if k == 0 else wbuf.at[k - 1, j]
        return pltpu.make_async_copy(src, wv.at[g, k], wl_sem.at[g, k])

    def out_copy(j):
        slot = lax.rem(j, 2)
        return remote(ov.at[slot], hbuf.at[j], o_send.at[slot], o_recv.at[j], bcore)

    def out_rows(i):
        shift = lax.div(i + 1, 2) * (2 * lax.rem(i, 2) - 1)
        q = lax.rem(y + shift + ny, ny)
        return pl.ds(pl.multiple_of(q * quarter, 16), quarter)

    def out_part(j, i):
        slot, rs = lax.rem(j, 2), out_rows(i)
        return remote(ov.at[slot, rs], hbuf.at[j, rs], o_send.at[slot], o_recv.at[j], bcore)

    def r_load(j):
        return pltpu.make_async_copy(r.at[:, wcol(j)], rv, r_sem)

    def block_product(lhs, rhs):
        return jnp.dot(lhs, rhs, preferred_element_type=jnp.float32).astype(jnp.bfloat16)

    def summed(g, rs):
        acc = None
        for k in range(4):
            prod = block_product(av[g, k, rs, :], wv[g, k]).astype(jnp.float32)
            acc = prod if acc is None else acc + prod
        return acc

    def gemm_out(j):
        slot = lax.rem(j, 2)

        def step(i, carry):
            @pl.when((j == 0) & (i == ny - 1))
            def _():
                a_fourth(0)

            rs = out_rows(i)
            ov[slot, rs, :] = summed(0, rs)

            @pl.when(i >= 1)
            def _():
                out_part(j, i - 1).start()

            return carry

        lax.fori_loop(0, ny, step, 0)

    def gemm_own():
        def step(i, carry):
            rs = pl.ds(pl.multiple_of(i * tile, tile), tile)
            lv[rs, :] = summed(1, rs)
            return carry

        lax.fori_loop(0, rows // tile, step, 0)

    items = ((xb, 0), (xb, 1), (xab, 0), (xab, 1), (x, o), (xa, o), (x, c), (xa, c))

    def at_load(n):
        pos, core = items[n]
        return pltpu.make_async_copy(a.at[arow(pos * CORES + core)], at.at[n % 2], at_sem.at[n % 2])

    def item_send(n):
        if n < 4:
            slot = n // 2 * 2 + c
            device = {"tp": xb * CORES + n % 2}
            return remote(pv.at[n], sb.at[slot], sb_send.at[n], sb_recv.at[slot], device)
        return remote(pv.at[n], sp.at[n - 4], sp_send.at[n - 4], sp_recv.at[n - 4], part)

    def item(n):
        at_load(n).wait()

        def step(i, carry):
            rs = pl.ds(pl.multiple_of(i * tile, tile), tile)
            pv[n, rs, :] = block_product(at[n % 2, rs, :], wv[0, 0])
            return carry

        lax.fori_loop(0, rows // tile, step, 0)
        if n + 2 < len(items):
            at_load(n + 2).start()

    def sb_arrival(slot):
        return remote(pv.at[0], sb.at[slot], sb_send.at[0], sb_recv.at[slot], bcore)

    def sf_copy():
        return remote(sg, hbuf.at[last], sf_send, sf_recv, acore)

    def for_rows(body):
        def step(t, carry):
            body(pl.ds(pl.multiple_of(t * 64, 64), 64))
            return carry

        lax.fori_loop(0, rows // 64, step, 0)

    def finish(j, rs, h):
        hbuf[j, rs, :] = h
        sq = h * h
        acc = ssacc[rs, :]
        for l in range(CN // 128):
            acc = acc + sq[:, l * 128:(l + 1) * 128]
        ssacc[rs, :] = acc

    def wide(v):
        return v.astype(jnp.float32)

    barrier = pltpu.get_barrier_semaphore()
    peers = [part, acore, aother, bcore, bother] + [{"tp2": lax.rem(y + d, ny)} for d in range(1, ny)]
    for peer in peers:
        pl.semaphore_signal(barrier, inc=1, device_id=peer, device_id_type=MESH)
    w_last = pltpu.make_async_copy(w.at[:, wcol(last)], wv.at[0, 0], wl_sem.at[0, 0])
    w_last.start()
    at_load(0).start()
    at_load(1).start()
    pl.semaphore_wait(barrier, len(peers))

    for t in range(PIECES):
        for s in range(2):
            a_cross(0, s, t).start()
    a_part(0).start()
    for j in range(AHEAD):
        w_cross(j).start()
        w_part(j).start()
        if j == 3:
            a_send(1, 0)
        if j == 6:
            a_send(1, 1)
    a_part(1).start()
    w_last.wait()
    with jax.named_scope("items"):
        item(0)
        item(1)
        item_send(0).start()
        item(2)
        item_send(1).start()
        item(3)
        item_send(2).start()
    a_local(0).start()
    a_local(1).start()
    ssacc[...] = jnp.zeros_like(ssacc)
    item_send(3).start()
    with jax.named_scope("a0_first"):
        for t in range(PIECES):
            for s in range(2):
                a_first(0, s, t)
    with jax.named_scope("items_2"):
        for n in range(4, 8):
            item(n)
        item_send(4).start()
        item_send(5).start()
    with jax.named_scope("a0_second"):
        for t in range(PIECES):
            for s in range(2):
                a_second(0, s, t)
    with jax.named_scope("a0_third"):
        a_third(0)

    def merge_last():
        r_load(last).start()
        sb_arrival(0).wait_recv()
        sb_arrival(1).wait_recv()
        with jax.named_scope("sf_wait"):
            sf_copy().wait_recv()
        r_load(last).wait()
        for_rows(lambda rs: finish(last, rs, wide(rv[rs, :]) + (
            (wide(pv[6, rs, :]) + wide(sp[0, rs, :])) + (wide(sb[0, rs, :]) + wide(sb[1, rs, :])) + hbuf[last, rs, :])))

    def sum_last():
        for n in range(2):
            item_send(4 + n).wait_recv()
            sb_arrival(2 + n).wait_recv()

        def body(rs):
            sg[rs, :] = (wide(pv[7, rs, :]) + wide(sp[1, rs, :])) + (wide(sb[2, rs, :]) + wide(sb[3, rs, :]))

        for_rows(body)

    def step(j, carry):
        @pl.when(j < last)
        def _():
            with jax.named_scope("w_cross_wait"):
                w_cross(j).wait_recv()
            w_pass(j).start()

            @pl.when(j + AHEAD < last)
            def _():
                w_cross(j + AHEAD).start()
                w_part(j + AHEAD).start()

            w_load(0, j, 0).start()
            w_load(0, j, 2).start()
            with jax.named_scope("w_pass_wait"):
                w_part(j).wait_recv()
                w_load(0, j, 1).start()
                w_pass(j).wait_recv()
                w_load(0, j, 3).start()

            @pl.when(j >= 2)
            def _():
                with jax.named_scope("o_send_wait"):
                    out_copy(j - 2).wait_send()

            with jax.named_scope("w_load_wait"):
                for k in range(4):
                    w_load(0, j, k).wait()
            with jax.named_scope("gemm0"):
                gemm_out(j)

            @pl.when(j == LAG)
            def _():
                for k in range(4):
                    w_load(1, 0, k).start()

            out_part(j, ny - 1).start()

        @pl.when(j == 4)
        def _():
            with jax.named_scope("a1_4"):
                for t in range(PIECES):
                    a_first(1, 0, t)

        @pl.when(j == LAG - 1)
        def _():
            with jax.named_scope("a1_6"):
                for t in range(PIECES):
                    a_second(1, 0, t)
                for t in range(PIECES):
                    a_first(1, 1, t)

        @pl.when(j == LAG)
        def _():
            with jax.named_scope("a1_7"):
                for t in range(PIECES):
                    a_second(1, 1, t)
                a_third(1)
                a_fourth(1)

        @pl.when(j == last - 3)
        def _():
            with jax.named_scope("sum_last"):
                sum_last()

        @pl.when(j == last)
        def _():
            with jax.named_scope("drain"):
                drain()

        @pl.when(j == last + 1)
        def _():
            with jax.named_scope("merge_last"):
                merge_last()

        def own(i, inner):
            r_load(i).start()
            with jax.named_scope("local_load_wait"):
                for k in range(4):
                    w_load(1, i, k).wait()
            with jax.named_scope("gemm1"):
                gemm_own()

            @pl.when(i + 1 < last)
            def _():
                for k in range(4):
                    w_load(1, i + 1, k).start()

            r_load(i).wait()
            with jax.named_scope("o_recv_wait"):
                out_copy(i).wait_recv()
            with jax.named_scope("merge"):
                for_rows(lambda rs: finish(i, rs, wide(rv[rs, :]) + (lv[rs, :] + hbuf[i, rs, :])))
            return inner

        @pl.when(j >= LAG)
        def _():
            n = 2 * (j - LAG)
            lax.fori_loop(jnp.maximum(n - 1, 0), jnp.minimum(n + 1, last), own, 0)

        @pl.when(j == last - 3)
        def _():
            sf_copy().start()

        return carry

    def drain():
        def body(j, carry):
            w_cross(j).wait_send()
            w_part(j).wait_send()
            w_pass(j).wait_send()
            return carry

        lax.fori_loop(0, last, body, 0)
        for g in range(2):
            a_part(g).wait_send()
            for s in range(2):
                for t in range(PIECES):
                    a_cross(g, s, t).wait_send()
                    a_far(g, s, t).wait_send()
                    for d in range(2):
                        a_near(g, s, t, d).wait_send()
        for n in range(6):
            item_send(n).wait_send()

    lax.fori_loop(0, LAG + (last + 1) // 2, step, 0)

    with jax.named_scope("sums"):
        svr[y] = lax.dot_general(jnp.ones((8, 128), jnp.float32), ssacc[...], (((1,), (1,)), ((), ())),
                                 preferred_element_type=jnp.float32, precision=lax.Precision.HIGHEST)
        sf_copy().wait_send()
        out_copy(last - 2).wait_send()
        out_copy(last - 1).wait_send()
    with jax.named_scope("sums_exchange"):
        sums = [remote(svr.at[y], svr.at[y], s_send.at[d - 1], s_recv.at[d - 1], {"tp2": lax.rem(y + d, ny)})
                for d in range(1, ny)]
        for copy in sums:
            copy.start()
        for d in range(1, ny):
            src = lax.rem(y + ny - d, ny)
            remote(svr.at[src], svr.at[src], s_send.at[d - 1], s_recv.at[d - 1], part).wait_recv()
        total = svr[0]
        for q in range(1, ny):
            total = total + svr[q]
        ssq_out[...] = total
        for copy in sums:
            copy.wait_send()


def norm_kernel(width, h, ssq, gain, hidden, normed, scale, hs, ns, h_sem, n_sem):
    chunks, rows, cols = h.shape
    inv_rms = lax.rsqrt(ssq[...] / width + EPS_NORM)
    scale[...] = jnp.broadcast_to(jnp.transpose(inv_rms)[:, :1], scale.shape)

    def copies(j):
        slot = lax.rem(j, 2)
        cs = pl.ds(pl.multiple_of(j * cols, cols), cols)
        return (pltpu.make_async_copy(hs.at[slot], hidden.at[:, cs], h_sem.at[slot]),
                pltpu.make_async_copy(ns.at[slot], normed.at[:, cs], n_sem.at[slot]))

    def chunk(j, carry):
        slot = lax.rem(j, 2)

        @pl.when(j >= 2)
        def _():
            for copy in copies(j - 2):
                copy.wait()

        g = gain[:, pl.ds(pl.multiple_of(j * cols, cols), cols)]

        def step(t, inner):
            rs = pl.ds(pl.multiple_of(t * 64, 64), 64)
            value = h[j, rs, :]
            hs[slot, rs, :] = value.astype(jnp.bfloat16)
            ns[slot, rs, :] = (value * scale[rs, :] * g).astype(jnp.bfloat16)
            return inner

        lax.fori_loop(0, rows // 64, step, 0)
        for copy in copies(j):
            copy.start()
        return carry

    lax.fori_loop(0, chunks, chunk, 0)
    for j in (chunks - 2, chunks - 1):
        for copy in copies(j):
            copy.wait()


def solution(mesh):
    tp, ny = mesh.shape["tp"], mesh.shape["tp2"]
    chips = tp // CORES

    def local_step(a, w, r, gain):
        depth, cols = w.shape
        rows = r.shape[0]
        last = cols // CN - 1
        dma = pltpu.SemaphoreType.DMA
        any_space = pl.BlockSpec(memory_space=pl.ANY)
        bf16, f32 = jnp.bfloat16, jnp.float32
        chunks = last + 1
        vmem = pl.BlockSpec(memory_space=pltpu.VMEM)
        h, ssq, _ = pl.pallas_call(
            functools.partial(kernel, ny, chips),
            out_shape=(
                pltpu.VMEM((chunks, rows, CN), f32),
                pltpu.VMEM((8, rows), f32),
                jax.ShapeDtypeStruct((3, last, depth, CN), bf16),
            ),
            in_specs=[any_space] * 3,
            out_specs=(vmem, vmem, any_space),
            scratch_shapes=[
                pltpu.VMEM((2, 4, rows, depth), bf16),
                pltpu.VMEM((2, 4, depth, CN), bf16),
                pltpu.VMEM((2, rows, CN), f32),
                pltpu.VMEM((rows, CN), f32),
                pltpu.VMEM((rows, CN), bf16),
                pltpu.VMEM((rows, 128), f32),
                pltpu.VMEM((ny, 8, rows), f32),
                pltpu.VMEM((2, rows, depth), bf16),
                pltpu.VMEM((8, rows, CN), bf16),
                pltpu.VMEM((4, rows, CN), bf16),
                pltpu.VMEM((2, rows, CN), bf16),
                pltpu.VMEM((rows, CN), f32),
                dma((2,)), dma((2,)), dma((2,)), dma((2, 2, PIECES)), dma((2, 2, PIECES)),
                dma((2, 2, PIECES, 2)), dma((2, 2, PIECES, 2)), dma((2, 2, PIECES)), dma((2, 2, PIECES)),
                dma((last,)), dma((last,)), dma((last,)), dma((last,)), dma((last,)), dma((last,)),
                dma((2,)), dma((last,)),
                dma((2, 4)), dma(()), dma((ny - 1,)), dma((ny - 1,)),
                dma((2,)), dma((4,)), dma((4,)), dma((2,)), dma((2,)), dma(()), dma(()),
            ],
            compiler_params=pltpu.CompilerParams(
                collective_id=0, has_side_effects=True, vmem_limit_bytes=54400000),
            cost_estimate=pl.CostEstimate(
                flops=2 * 8 * rows * depth * cols, bytes_accessed=8 * depth * cols * 2, transcendentals=0),
        )(a, w, r)
        return pl.pallas_call(
            functools.partial(norm_kernel, cols * ny),
            out_shape=(jax.ShapeDtypeStruct((rows, cols), bf16),) * 2,
            in_specs=[vmem] * 3,
            out_specs=(any_space, any_space),
            scratch_shapes=[
                pltpu.VMEM((rows, CN), f32), pltpu.VMEM((2, rows, CN), bf16), pltpu.VMEM((2, rows, CN), bf16),
                dma((2,)), dma((2,)),
            ],
            compiler_params=pltpu.CompilerParams(vmem_limit_bytes=24 << 20),
            cost_estimate=pl.CostEstimate(flops=4 * rows * cols, bytes_accessed=8 * rows * cols, transcendentals=rows),
        )(pltpu.with_memory_space_constraint(h, pltpu.VMEM), pltpu.with_memory_space_constraint(ssq, pltpu.VMEM), gain.reshape(1, cols))

    row_spec = P(("dp", "tp"), "tp2")
    return jax.shard_map(local_step, mesh=mesh, in_specs=(P("dp", "tp"), P("tp", "tp2"), row_spec, P("tp2")),
                         out_specs=(row_spec, row_spec), check_vma=False)
```

```python
import functools

import jax
import jax.numpy as jnp
from jax import lax
from jax.experimental import pallas as pl
from jax.experimental.pallas import tpu as pltpu
from jax.sharding import PartitionSpec as P

EPS_NORM = 1e-6
MESH = pl.DeviceIdType.MESH
CORES = 2
CN = 256
LAG = 7
AHEAD = 7
PIECES = 4


def kernel(ny, chips, a, w, r, hbuf, ssq_out, wbuf, av, wv, ov, lv, rv, ssacc, svr, at, pv, sb, sp, sg,
           al_sem, ap_send, ap_recv, ax_send, ax_recv, ay_send, ay_recv, af_send, af_recv,
           wp_send, wp_recv, wa_send, wa_recv, wf_send, wf_recv, o_send, o_recv,
           wl_sem, r_sem, s_send, s_recv, at_sem, sb_send, sb_recv, sp_send, sp_recv, sf_send, sf_recv):
    rows, cols = r.shape
    last = cols // CN - 1
    quarter = rows // ny
    piece = quarter // PIECES
    tile = min(256, rows)
    me, y = lax.axis_index("tp"), lax.axis_index("tp2")
    x, c = lax.div(me, CORES), lax.rem(me, CORES)
    o = 1 - c
    xa = x + 1 - 2 * lax.rem(x, 2)
    xb = chips - 1 - x
    xab = chips - 1 - xa
    yp, ym = lax.rem(y + 1, ny), lax.rem(y + ny - 1, ny)
    part = {"tp": x * CORES + o}
    acore, aother = {"tp": xa * CORES + c}, {"tp": xa * CORES + o}
    bcore, bother = {"tp": xb * CORES + c}, {"tp": xb * CORES + o}
    up, down = {"tp2": yp}, {"tp2": ym}

    def remote(src, dst, send, recv, device):
        return pltpu.make_async_remote_copy(
            src_ref=src, dst_ref=dst, send_sem=send, recv_sem=recv, device_id=device, device_id_type=MESH)

    def arow(owner, size=None, shift=0):
        return pl.ds(pl.multiple_of(owner * rows + shift, 16), rows if size is None else size)

    def qrow(q, t):
        return pl.ds(pl.multiple_of(q * quarter + t * piece, 16), piece)

    def wcol(j):
        return pl.ds(pl.multiple_of(j * CN, CN), CN)

    own_rows = (xb * CORES + c, me)
    part_rows = (xb * CORES + o, x * CORES + o)

    def a_local(g):
        return pltpu.make_async_copy(a.at[arow(own_rows[g])], av.at[g, 0], al_sem.at[g])

    def a_part(g):
        return remote(a.at[arow(part_rows[g])], av.at[g, 1], ap_send.at[g], ap_recv.at[g], part)

    def a_cross(g, s, t):
        core, device = ((c, acore), (o, aother))[s]
        owner = (xab, xa)[g] * CORES + core
        return remote(a.at[arow(owner, piece, y * quarter + t * piece)], av.at[g, 2 + s, qrow(y, t)],
                      ax_send.at[g, s, t], ax_recv.at[g, s, t], device)

    def a_near(g, s, t, d):
        ref = av.at[g, 2 + s, qrow(y, t)]
        return remote(ref, ref, ay_send.at[g, s, t, d], ay_recv.at[g, s, t, d], (up, down)[d])

    def a_far(g, s, t):
        ref = av.at[g, 2 + s, qrow((ym, yp)[s], t)]
        return remote(ref, ref, af_send.at[g, s, t], af_recv.at[g, s, t], (up, down)[s])

    halves = (range(PIECES // 2), range(PIECES // 2, PIECES))

    def a_first(g, s, t):
        a_cross(g, s, t).wait_recv()
        for d in range(2):
            a_near(g, s, t, d).start()

    def a_second(g, s, t):
        a_near(g, s, t, s).wait_recv()
        a_far(g, s, t).start()

    def a_third(g, ts):
        for t in ts:
            for s in range(2):
                a_near(g, s, t, 1 - s).wait_recv()

    def a_fourth(g, ts):
        for t in ts:
            for s in range(2):
                a_far(g, s, t).wait_recv()

    def w_part(j):
        return remote(w.at[:, wcol(j)], wbuf.at[0, j], wp_send.at[j], wp_recv.at[j], part)

    def w_cross(j):
        return remote(w.at[:, wcol(j)], wbuf.at[1, j], wa_send.at[j], wa_recv.at[j], acore)

    def w_pass(j):
        return remote(wbuf.at[1, j], wbuf.at[2, j], wf_send.at[j], wf_recv.at[j], part)

    def w_load(g, j, k):
        src = w.at[:, wcol(j)] if k == 0 else wbuf.at[k - 1, j]
        return pltpu.make_async_copy(src, wv.at[g, k], wl_sem.at[g, k])

    def out_copy(j):
        slot = lax.rem(j, 2)
        return remote(ov.at[slot], hbuf.at[j], o_send.at[slot], o_recv.at[j], bcore)

    def out_rows(i):
        half, k = lax.div(i, ny), lax.rem(i, ny)
        shift = lax.div(k + 1, 2) * (2 * lax.rem(k, 2) - 1)
        q = lax.rem(y + shift + ny, ny)
        return pl.ds(pl.multiple_of(q * quarter + half * (quarter // 2), 16), quarter // 2)

    def out_part(j, i):
        slot, rs = lax.rem(j, 2), out_rows(i)
        return remote(ov.at[slot, rs], hbuf.at[j, rs], o_send.at[slot], o_recv.at[j], bcore)

    def r_load(j):
        return pltpu.make_async_copy(r.at[:, wcol(j)], rv, r_sem)

    def block_product(lhs, rhs):
        return jnp.dot(lhs, rhs, preferred_element_type=jnp.float32).astype(jnp.bfloat16)

    def summed(g, rs):
        acc = None
        for k in range(4):
            prod = block_product(av[g, k, rs, :], wv[g, k]).astype(jnp.float32)
            acc = prod if acc is None else acc + prod
        return acc

    def gemm_out(j):
        slot = lax.rem(j, 2)

        def step(i, carry):
            @pl.when((j == 0) & (i == ny - 1))
            def _():
                a_fourth(0, halves[0])

            @pl.when((j == 0) & (i == ny))
            def _():
                with jax.named_scope("a0_half"):
                    for t in halves[1]:
                        for s in range(2):
                            a_first(0, s, t)
                    for t in halves[1]:
                        for s in range(2):
                            a_second(0, s, t)
                    a_third(0, halves[1])

            @pl.when((j == 0) & (i == 2 * ny - 1))
            def _():
                with jax.named_scope("a0_far"):
                    a_fourth(0, halves[1])

            rs = out_rows(i)
            ov[slot, rs, :] = summed(0, rs)

            @pl.when(i >= 1)
            def _():
                out_part(j, i - 1).start()

            return carry

        lax.fori_loop(0, 2 * ny, step, 0)

    def gemm_own():
        def step(i, carry):
            rs = pl.ds(pl.multiple_of(i * tile, tile), tile)
            lv[rs, :] = summed(1, rs)
            return carry

        lax.fori_loop(0, rows // tile, step, 0)

    items = ((xb, 0), (xb, 1), (xab, 0), (xab, 1), (x, o), (xa, o), (x, c), (xa, c))

    def at_load(n):
        pos, core = items[n]
        return pltpu.make_async_copy(a.at[arow(pos * CORES + core)], at.at[n % 2], at_sem.at[n % 2])

    def item_send(n):
        if n < 4:
            slot = n // 2 * 2 + c
            device = {"tp": xb * CORES + n % 2}
            return remote(pv.at[n], sb.at[slot], sb_send.at[n], sb_recv.at[slot], device)
        return remote(pv.at[n], sp.at[n - 4], sp_send.at[n - 4], sp_recv.at[n - 4], part)

    def item(n):
        at_load(n).wait()

        def step(i, carry):
            rs = pl.ds(pl.multiple_of(i * tile, tile), tile)
            pv[n, rs, :] = block_product(at[n % 2, rs, :], wv[0, 0])
            return carry

        lax.fori_loop(0, rows // tile, step, 0)
        if n + 2 < len(items):
            at_load(n + 2).start()

    def sb_arrival(slot):
        return remote(pv.at[0], sb.at[slot], sb_send.at[0], sb_recv.at[slot], bcore)

    def sf_copy():
        return remote(sg, hbuf.at[last], sf_send, sf_recv, acore)

    def for_rows(body):
        def step(t, carry):
            body(pl.ds(pl.multiple_of(t * 64, 64), 64))
            return carry

        lax.fori_loop(0, rows // 64, step, 0)

    def finish(j, rs, h):
        hbuf[j, rs, :] = h
        sq = h * h
        acc = ssacc[rs, :]
        for l in range(CN // 128):
            acc = acc + sq[:, l * 128:(l + 1) * 128]
        ssacc[rs, :] = acc

    def wide(v):
        return v.astype(jnp.float32)

    barrier = pltpu.get_barrier_semaphore()
    peers = [part, acore, aother, bcore, bother] + [{"tp2": lax.rem(y + d, ny)} for d in range(1, ny)]
    for peer in peers:
        pl.semaphore_signal(barrier, inc=1, device_id=peer, device_id_type=MESH)
    w_last = pltpu.make_async_copy(w.at[:, wcol(last)], wv.at[0, 0], wl_sem.at[0, 0])
    w_last.start()
    at_load(0).start()
    at_load(1).start()
    w_last.wait()
    item(0)
    pl.semaphore_wait(barrier, len(peers))

    for t in halves[0]:
        for s in range(2):
            a_cross(0, s, t).start()
    a_part(0).start()
    for j in range(AHEAD):
        w_cross(j).start()
        w_part(j).start()
        if j == 0:
            for t in halves[1]:
                for s in range(2):
                    a_cross(0, s, t).start()
        if j in (3, 6):
            for t in range(PIECES):
                a_cross(1, j // 6, t).start()
    a_part(1).start()
    item_send(0).start()
    with jax.named_scope("items"):
        item(1)
        item(2)
        item_send(1).start()
        item(3)
        item_send(2).start()
    a_local(0).start()
    a_local(1).start()
    ssacc[...] = jnp.zeros_like(ssacc)
    item_send(3).start()
    with jax.named_scope("a0_first"):
        for t in halves[0]:
            for s in range(2):
                a_first(0, s, t)
    with jax.named_scope("items_2"):
        for n in range(4, 8):
            item(n)
        item_send(4).start()
        item_send(5).start()
    with jax.named_scope("a0_second"):
        for t in halves[0]:
            for s in range(2):
                a_second(0, s, t)
    with jax.named_scope("a0_third"):
        a_local(0).wait()
        a_part(0).wait_recv()
        a_third(0, halves[0])

    def merge_last():
        r_load(last).start()
        sb_arrival(0).wait_recv()
        sb_arrival(1).wait_recv()
        with jax.named_scope("sf_wait"):
            sf_copy().wait_recv()
        r_load(last).wait()
        for_rows(lambda rs: finish(last, rs, wide(rv[rs, :]) + (
            (wide(pv[6, rs, :]) + wide(sp[0, rs, :])) + (wide(sb[0, rs, :]) + wide(sb[1, rs, :])) + hbuf[last, rs, :])))

    def sum_last():
        for n in range(2):
            item_send(4 + n).wait_recv()
            sb_arrival(2 + n).wait_recv()

        def body(rs):
            sg[rs, :] = (wide(pv[7, rs, :]) + wide(sp[1, rs, :])) + (wide(sb[2, rs, :]) + wide(sb[3, rs, :]))

        for_rows(body)

    def step(j, carry):
        @pl.when(j < last)
        def _():
            with jax.named_scope("w_cross_wait"):
                w_cross(j).wait_recv()
            w_pass(j).start()

            @pl.when(j + AHEAD < last)
            def _():
                w_cross(j + AHEAD).start()
                w_part(j + AHEAD).start()

            w_load(0, j, 0).start()
            w_load(0, j, 2).start()
            with jax.named_scope("w_pass_wait"):
                w_part(j).wait_recv()
                w_load(0, j, 1).start()
                w_pass(j).wait_recv()
                w_load(0, j, 3).start()

            @pl.when(j >= 2)
            def _():
                with jax.named_scope("o_send_wait"):
                    out_copy(j - 2).wait_send()

            with jax.named_scope("w_load_wait"):
                for k in range(4):
                    w_load(0, j, k).wait()
            with jax.named_scope("gemm0"):
                gemm_out(j)

            @pl.when(j == LAG)
            def _():
                for k in range(4):
                    w_load(1, 0, k).start()

            out_part(j, 2 * ny - 1).start()

        @pl.when(j == 3)
        def _():
            with jax.named_scope("a1_3"):
                for t in range(PIECES):
                    a_first(1, 0, t)

        @pl.when(j == 4)
        def _():
            with jax.named_scope("a1_4"):
                for t in range(PIECES):
                    a_second(1, 0, t)

        @pl.when(j == LAG - 1)
        def _():
            with jax.named_scope("a1_6"):
                for t in range(PIECES):
                    a_first(1, 1, t)
                for t in range(PIECES):
                    a_second(1, 1, t)

        @pl.when(j == LAG)
        def _():
            with jax.named_scope("a1_7"):
                a_local(1).wait()
                a_part(1).wait_recv()
                a_third(1, range(PIECES))
                a_fourth(1, range(PIECES))

        @pl.when(j == last - 3)
        def _():
            with jax.named_scope("sum_last"):
                sum_last()

        @pl.when(j == last)
        def _():
            with jax.named_scope("drain"):
                drain()

        @pl.when(j == last + 1)
        def _():
            with jax.named_scope("merge_last"):
                merge_last()

        def own(i, inner):
            r_load(i).start()
            with jax.named_scope("local_load_wait"):
                for k in range(4):
                    w_load(1, i, k).wait()
            with jax.named_scope("gemm1"):
                gemm_own()

            @pl.when(i + 1 < last)
            def _():
                for k in range(4):
                    w_load(1, i + 1, k).start()

            r_load(i).wait()
            with jax.named_scope("o_recv_wait"):
                out_copy(i).wait_recv()
            with jax.named_scope("merge"):
                for_rows(lambda rs: finish(i, rs, wide(rv[rs, :]) + (lv[rs, :] + hbuf[i, rs, :])))
            return inner

        @pl.when(j >= LAG)
        def _():
            n = 2 * (j - LAG)
            lax.fori_loop(jnp.maximum(n - 1, 0), jnp.minimum(n + 1, last), own, 0)

        @pl.when(j == last - 3)
        def _():
            sf_copy().start()

        return carry

    def drain():
        def body(j, carry):
            w_cross(j).wait_send()
            w_part(j).wait_send()
            w_pass(j).wait_send()
            return carry

        lax.fori_loop(0, last, body, 0)
        for g in range(2):
            a_part(g).wait_send()
            for s in range(2):
                for t in range(PIECES):
                    a_cross(g, s, t).wait_send()
                    a_far(g, s, t).wait_send()
                    for d in range(2):
                        a_near(g, s, t, d).wait_send()
        for n in range(6):
            item_send(n).wait_send()

    lax.fori_loop(0, LAG + (last + 1) // 2, step, 0)

    with jax.named_scope("sums"):
        svr[y] = lax.dot_general(jnp.ones((8, 128), jnp.float32), ssacc[...], (((1,), (1,)), ((), ())),
                                 preferred_element_type=jnp.float32, precision=lax.Precision.HIGHEST)
        sf_copy().wait_send()
        out_copy(last - 2).wait_send()
        out_copy(last - 1).wait_send()
    with jax.named_scope("sums_exchange"):
        sums = [remote(svr.at[y], svr.at[y], s_send.at[d - 1], s_recv.at[d - 1], {"tp2": lax.rem(y + d, ny)})
                for d in range(1, ny)]
        for copy in sums:
            copy.start()
        for d in range(1, ny):
            src = lax.rem(y + ny - d, ny)
            remote(svr.at[src], svr.at[src], s_send.at[d - 1], s_recv.at[d - 1], part).wait_recv()
        total = svr[0]
        for q in range(1, ny):
            total = total + svr[q]
        ssq_out[...] = total
        for copy in sums:
            copy.wait_send()


def norm_kernel(width, h, ssq, gain, hidden, normed, scale, hs, ns, h_sem, n_sem):
    chunks, rows, cols = h.shape
    span = hs.shape[1]
    inv_rms = lax.rsqrt(ssq[...] / width + EPS_NORM)
    scale[...] = jnp.broadcast_to(jnp.transpose(inv_rms)[:, :1], scale.shape)

    def row_block(t):
        return pl.ds(pl.multiple_of(t * span, span), span)

    def copies(t):
        slot = lax.rem(t, 2)
        return (pltpu.make_async_copy(hs.at[slot], hidden.at[row_block(t)], h_sem.at[slot]),
                pltpu.make_async_copy(ns.at[slot], normed.at[row_block(t)], n_sem.at[slot]))

    def block(t, carry):
        slot, rs = lax.rem(t, 2), row_block(t)

        @pl.when(t >= 2)
        def _():
            for copy in copies(t - 2):
                copy.wait()

        factor = scale[rs, :]
        for j in range(chunks):
            cs = slice(j * cols, (j + 1) * cols)
            value = h[j, rs, :]
            hs[slot, :, cs] = value.astype(jnp.bfloat16)
            ns[slot, :, cs] = (value * factor * gain[:, cs]).astype(jnp.bfloat16)
        for copy in copies(t):
            copy.start()
        return carry

    blocks = rows // span
    lax.fori_loop(0, blocks, block, 0)
    for t in (blocks - 2, blocks - 1):
        for copy in copies(t):
            copy.wait()


def solution(mesh):
    tp, ny = mesh.shape["tp"], mesh.shape["tp2"]
    chips = tp // CORES

    def local_step(a, w, r, gain):
        depth, cols = w.shape
        rows = r.shape[0]
        last = cols // CN - 1
        dma = pltpu.SemaphoreType.DMA
        any_space = pl.BlockSpec(memory_space=pl.ANY)
        bf16, f32 = jnp.bfloat16, jnp.float32
        chunks = last + 1
        vmem = pl.BlockSpec(memory_space=pltpu.VMEM)
        h, ssq, _ = pl.pallas_call(
            functools.partial(kernel, ny, chips),
            out_shape=(
                pltpu.VMEM((chunks, rows, CN), f32),
                pltpu.VMEM((8, rows), f32),
                jax.ShapeDtypeStruct((3, last, depth, CN), bf16),
            ),
            in_specs=[any_space] * 3,
            out_specs=(vmem, vmem, any_space),
            scratch_shapes=[
                pltpu.VMEM((2, 4, rows, depth), bf16),
                pltpu.VMEM((2, 4, depth, CN), bf16),
                pltpu.VMEM((2, rows, CN), f32),
                pltpu.VMEM((rows, CN), f32),
                pltpu.VMEM((rows, CN), bf16),
                pltpu.VMEM((rows, 128), f32),
                pltpu.VMEM((ny, 8, rows), f32),
                pltpu.VMEM((2, rows, depth), bf16),
                pltpu.VMEM((8, rows, CN), bf16),
                pltpu.VMEM((4, rows, CN), bf16),
                pltpu.VMEM((2, rows, CN), bf16),
                pltpu.VMEM((rows, CN), f32),
                dma((2,)), dma((2,)), dma((2,)), dma((2, 2, PIECES)), dma((2, 2, PIECES)),
                dma((2, 2, PIECES, 2)), dma((2, 2, PIECES, 2)), dma((2, 2, PIECES)), dma((2, 2, PIECES)),
                dma((last,)), dma((last,)), dma((last,)), dma((last,)), dma((last,)), dma((last,)),
                dma((2,)), dma((last,)),
                dma((2, 4)), dma(()), dma((ny - 1,)), dma((ny - 1,)),
                dma((2,)), dma((4,)), dma((4,)), dma((2,)), dma((2,)), dma(()), dma(()),
            ],
            compiler_params=pltpu.CompilerParams(
                collective_id=0, has_side_effects=True, vmem_limit_bytes=54400000),
            cost_estimate=pl.CostEstimate(
                flops=2 * 8 * rows * depth * cols, bytes_accessed=8 * depth * cols * 2, transcendentals=0),
        )(a, w, r)
        return pl.pallas_call(
            functools.partial(norm_kernel, cols * ny),
            out_shape=(jax.ShapeDtypeStruct((rows, cols), bf16),) * 2,
            in_specs=[vmem] * 3,
            out_specs=(any_space, any_space),
            scratch_shapes=[
                pltpu.VMEM((rows, CN), f32), pltpu.VMEM((2, 64, cols), bf16), pltpu.VMEM((2, 64, cols), bf16),
                dma((2,)), dma((2,)),
            ],
            compiler_params=pltpu.CompilerParams(vmem_limit_bytes=24 << 20),
            cost_estimate=pl.CostEstimate(flops=4 * rows * cols, bytes_accessed=8 * rows * cols, transcendentals=rows),
        )(pltpu.with_memory_space_constraint(h, pltpu.VMEM), pltpu.with_memory_space_constraint(ssq, pltpu.VMEM), gain.reshape(1, cols))

    row_spec = P(("dp", "tp"), "tp2")
    return jax.shard_map(local_step, mesh=mesh, in_specs=(P("dp", "tp"), P("tp", "tp2"), row_spec, P("tp2")),
                         out_specs=(row_spec, row_spec), check_vma=False)
```

```python
import functools

import jax
import jax.numpy as jnp
from jax import lax
from jax.experimental import pallas as pl
from jax.experimental.pallas import tpu as pltpu
from jax.sharding import PartitionSpec as P

EPS_NORM = 1e-6
MESH = pl.DeviceIdType.MESH
CORES = 2
CN = 256
LAG = 7
AHEAD = 7
PIECES = 4


def kernel(ny, chips, a, w, r, hbuf, ssq_out, wbuf, av, wv, ov, lv, rv, ssacc, svr, at, pv, sb, sp, sg,
           al_sem, ap_send, ap_recv, ax_send, ax_recv, ay_send, ay_recv, ao_recv, af_send, af_recv,
           wp_send, wp_recv, wa_send, wa_recv, wf_send, wf_recv, o_send, o_recv,
           wl_sem, r_sem, s_send, s_recv, at_sem, sb_send, sb_recv, sp_send, sp_recv, sf_send, sf_recv):
    rows, cols = r.shape
    last = cols // CN - 1
    quarter = rows // ny
    piece = quarter // PIECES
    tile = min(256, rows)
    me, y = lax.axis_index("tp"), lax.axis_index("tp2")
    x, c = lax.div(me, CORES), lax.rem(me, CORES)
    o = 1 - c
    xa = x + 1 - 2 * lax.rem(x, 2)
    xb = chips - 1 - x
    xab = chips - 1 - xa
    yp, ym = lax.rem(y + 1, ny), lax.rem(y + ny - 1, ny)
    part = {"tp": x * CORES + o}
    acore, aother = {"tp": xa * CORES + c}, {"tp": xa * CORES + o}
    bcore, bother = {"tp": xb * CORES + c}, {"tp": xb * CORES + o}
    up, down = {"tp2": yp}, {"tp2": ym}

    def remote(src, dst, send, recv, device):
        return pltpu.make_async_remote_copy(
            src_ref=src, dst_ref=dst, send_sem=send, recv_sem=recv, device_id=device, device_id_type=MESH)

    def arow(owner, size=None, shift=0):
        return pl.ds(pl.multiple_of(owner * rows + shift, 16), rows if size is None else size)

    def qrow(q, t):
        return pl.ds(pl.multiple_of(q * quarter + t * piece, 16), piece)

    def wcol(j):
        return pl.ds(pl.multiple_of(j * CN, CN), CN)

    own_rows = (xb * CORES + c, me)
    part_rows = (xb * CORES + o, x * CORES + o)

    def a_local(g):
        return pltpu.make_async_copy(a.at[arow(own_rows[g])], av.at[g, 0], al_sem.at[g])

    def a_part(g):
        return remote(a.at[arow(part_rows[g])], av.at[g, 1], ap_send, ap_recv.at[g], part)

    def a_cross(g, s, t):
        core, device = ((c, acore), (o, aother))[s]
        owner = (xab, xa)[g] * CORES + core
        return remote(a.at[arow(owner, piece, y * quarter + t * piece)], av.at[g, 2 + s, qrow(y, t)],
                      ax_send, ax_recv.at[g, s, t], device)

    def a_near(g, s, t, d):
        ref = av.at[g, 2 + s, qrow(y, t)]
        recv = ay_recv.at[g, s, t] if d == s else ao_recv.at[g, t // (PIECES // 2)]
        return remote(ref, ref, ay_send, recv, (up, down)[d])

    def a_far(g, s, t):
        ref = av.at[g, 2 + s, qrow((ym, yp)[s], t)]
        return remote(ref, ref, af_send, af_recv.at[g, t // (PIECES // 2)], (up, down)[s])

    halves = (range(PIECES // 2), range(PIECES // 2, PIECES))

    def a_first(g, s, t):
        a_cross(g, s, t).wait_recv()
        for d in range(2):
            a_near(g, s, t, d).start()

    def a_second(g, s, t):
        a_near(g, s, t, s).wait_recv()
        a_far(g, s, t).start()

    def half_arrival(sem, g):
        ref = av.at[g, 2, pl.ds(0, quarter)]
        return remote(ref, ref, ay_send, sem, part)

    def a_third(g, half):
        half_arrival(ao_recv.at[g, half], g).wait_recv()

    def a_fourth(g, half):
        half_arrival(af_recv.at[g, half], g).wait_recv()

    def w_part(j):
        return remote(w.at[:, wcol(j)], wbuf.at[0, j], wp_send, wp_recv.at[j], part)

    def w_cross(j):
        return remote(w.at[:, wcol(j)], wbuf.at[1, j], wa_send, wa_recv.at[j], acore)

    def w_pass(j):
        return remote(wbuf.at[1, j], wbuf.at[2, j], wf_send, wf_recv.at[j], part)

    def w_load(g, j, k):
        src = w.at[:, wcol(j)] if k == 0 else wbuf.at[k - 1, j]
        return pltpu.make_async_copy(src, wv.at[g, k], wl_sem.at[g, k])

    def w_loads(g, j):
        for k in range(4):
            w_load(g, j, k).start()

    def out_copy(j):
        slot = lax.rem(j, 2)
        return remote(ov.at[slot], hbuf.at[j], o_send.at[slot], o_recv.at[j], bcore)

    def out_rows(i):
        half, k = lax.div(i, ny), lax.rem(i, ny)
        shift = lax.div(k + 1, 2) * (2 * lax.rem(k, 2) - 1)
        q = lax.rem(y + shift + ny, ny)
        return pl.ds(pl.multiple_of(q * quarter + half * (quarter // 2), 16), quarter // 2)

    def out_part(j, i):
        slot, rs = lax.rem(j, 2), out_rows(i)
        return remote(ov.at[slot, rs], hbuf.at[j, rs], o_send.at[slot], o_recv.at[j], bcore)

    def r_load(j):
        return pltpu.make_async_copy(r.at[:, wcol(j)], rv, r_sem)

    def block_product(lhs, rhs):
        return jnp.dot(lhs, rhs, preferred_element_type=jnp.float32).astype(jnp.bfloat16)

    def summed(g, buf, rs):
        acc = None
        for k in range(4):
            prod = block_product(av[g, k, rs, :], wv[buf, k]).astype(jnp.float32)
            acc = prod if acc is None else acc + prod
        return acc

    def gemm_out(j):
        slot = lax.rem(j, 2)
        late = (j == 0) | (j == 4) | (j == LAG)

        def step(i, carry):
            @pl.when((j == 0) & (i == ny - 1))
            def _():
                a_fourth(0, 0)

            @pl.when((j == 0) & (i == ny))
            def _():
                with jax.named_scope("a0_half"):
                    for t in halves[1]:
                        for s in range(2):
                            a_first(0, s, t)
                    for t in halves[1]:
                        for s in range(2):
                            a_second(0, s, t)
                    a_third(0, 1)

            @pl.when((j == 0) & (i == 2 * ny - 1))
            def _():
                with jax.named_scope("a0_far"):
                    a_fourth(0, 1)

            rs = out_rows(i)
            ov[slot, rs, :] = summed(0, 0, rs)

            @pl.when((i >= 1) & late)
            def _():
                out_part(j, i - 1).start()

            return carry

        lax.fori_loop(0, 2 * ny, step, 0)

    def gemm_own(buf):
        def step(i, carry):
            rs = pl.ds(pl.multiple_of(i * tile, tile), tile)
            lv[rs, :] = summed(1, buf, rs)
            return carry

        lax.fori_loop(0, rows // tile, step, 0)

    items = ((xb, 0), (xb, 1), (xab, 0), (xab, 1), (x, o), (xa, o), (x, c), (xa, c))

    def at_load(n):
        pos, core = items[n]
        return pltpu.make_async_copy(a.at[arow(pos * CORES + core)], at.at[n % 2], at_sem.at[n % 2])

    def item_send(n):
        if n < 4:
            slot = n // 2 * 2 + c
            device = {"tp": xb * CORES + n % 2}
            return remote(pv.at[n], sb.at[slot], sb_send, sb_recv.at[slot], device)
        return remote(pv.at[n], sp.at[n - 4], sp_send, sp_recv.at[n - 4], part)

    def item(n):
        at_load(n).wait()

        def step(i, carry):
            rs = pl.ds(pl.multiple_of(i * tile, tile), tile)
            pv[n, rs, :] = block_product(at[n % 2, rs, :], wv[0, 0])
            return carry

        lax.fori_loop(0, rows // tile, step, 0)
        if n + 2 < len(items):
            at_load(n + 2).start()

    def sb_arrival(slot):
        return remote(pv.at[0], sb.at[slot], sb_send, sb_recv.at[slot], bcore)

    def sf_copy():
        return remote(sg, hbuf.at[last], sf_send, sf_recv, acore)

    def for_rows(body):
        def step(t, carry):
            body(pl.ds(pl.multiple_of(t * 64, 64), 64))
            return carry

        lax.fori_loop(0, rows // 64, step, 0)

    def finish(j, rs, h):
        hbuf[j, rs, :] = h
        sq = h * h
        acc = ssacc[rs, :]
        for l in range(CN // 128):
            acc = acc + sq[:, l * 128:(l + 1) * 128]
        ssacc[rs, :] = acc

    def wide(v):
        return v.astype(jnp.float32)

    barrier = pltpu.get_barrier_semaphore()
    peers = [part, acore, aother, bcore, bother] + [{"tp2": lax.rem(y + d, ny)} for d in range(1, ny)]
    for peer in peers:
        pl.semaphore_signal(barrier, inc=1, device_id=peer, device_id_type=MESH)
    w_last = pltpu.make_async_copy(w.at[:, wcol(last)], wv.at[0, 0], wl_sem.at[0, 0])
    w_last.start()
    at_load(0).start()
    at_load(1).start()
    pl.semaphore_wait(barrier, len(peers))

    for t in halves[0]:
        for s in range(2):
            a_cross(0, s, t).start()
    a_part(0).start()
    for j in range(AHEAD):
        w_cross(j).start()
        w_part(j).start()
        if j == 0:
            for t in halves[1]:
                for s in range(2):
                    a_cross(0, s, t).start()
        if j in (3, 6):
            for t in range(PIECES):
                a_cross(1, j // 6, t).start()
    a_part(1).start()
    w_last.wait()
    with jax.named_scope("items"):
        item(0)
        item(1)
        item_send(0).start()
        item(2)
        item_send(1).start()
        item(3)
        item_send(2).start()
    a_local(0).start()
    a_local(1).start()
    ssacc[...] = jnp.zeros_like(ssacc)
    item_send(3).start()
    with jax.named_scope("a0_first"):
        for t in halves[0]:
            for s in range(2):
                a_first(0, s, t)
    with jax.named_scope("items_2"):
        for n in range(4, 8):
            item(n)
        item_send(4).start()
        item_send(5).start()
    with jax.named_scope("a0_second"):
        for t in halves[0]:
            for s in range(2):
                a_second(0, s, t)
    with jax.named_scope("a0_third"):
        a_local(0).wait()
        a_part(0).wait_recv()
        a_third(0, 0)

    def merge_last():
        r_load(last).start()
        sb_arrival(0).wait_recv()
        sb_arrival(1).wait_recv()
        with jax.named_scope("sf_wait"):
            sf_copy().wait_recv()
        r_load(last).wait()
        for_rows(lambda rs: finish(last, rs, wide(rv[rs, :]) + (
            (wide(pv[6, rs, :]) + wide(sp[0, rs, :])) + (wide(sb[0, rs, :]) + wide(sb[1, rs, :])) + hbuf[last, rs, :])))

    def sum_last():
        for n in range(2):
            item_send(4 + n).wait_recv()
            sb_arrival(2 + n).wait_recv()

        def body(rs):
            sg[rs, :] = (wide(pv[7, rs, :]) + wide(sp[1, rs, :])) + (wide(sb[2, rs, :]) + wide(sb[3, rs, :]))

        for_rows(body)

    def step(j, carry):
        @pl.when(j < last)
        def _():
            with jax.named_scope("w_cross_wait"):
                w_cross(j).wait_recv()
            w_pass(j).start()

            @pl.when(j + AHEAD < last)
            def _():
                w_cross(j + AHEAD).start()
                w_part(j + AHEAD).start()

            w_load(0, j, 0).start()
            w_load(0, j, 2).start()
            with jax.named_scope("w_pass_wait"):
                w_part(j).wait_recv()
                w_load(0, j, 1).start()
                w_pass(j).wait_recv()
                w_load(0, j, 3).start()

            @pl.when(j >= 2)
            def _():
                with jax.named_scope("o_send_wait"):
                    out_copy(j - 2).wait_send()

            with jax.named_scope("w_load_wait"):
                for k in range(4):
                    w_load(0, j, k).wait()
            with jax.named_scope("gemm0"):
                gemm_out(j)

            late = (j == 0) | (j == 4) | (j == LAG)

            @pl.when(late)
            def _():
                out_part(j, 2 * ny - 1).start()

            @pl.when(jnp.logical_not(late))
            def _():
                out_copy(j).start()

        @pl.when(j == LAG)
        def _():
            w_loads(1, 1)

        @pl.when((j >= LAG) & (2 * (j - LAG) < last))
        def _():
            w_loads(0, 2 * (j - LAG))

        @pl.when(j == 3)
        def _():
            with jax.named_scope("a1_3"):
                for t in range(PIECES):
                    a_first(1, 0, t)

        @pl.when(j == 4)
        def _():
            with jax.named_scope("a1_4"):
                for t in range(PIECES):
                    a_second(1, 0, t)

        @pl.when(j == LAG - 1)
        def _():
            with jax.named_scope("a1_6"):
                for t in range(PIECES):
                    a_first(1, 1, t)
                for t in range(PIECES):
                    a_second(1, 1, t)

        @pl.when(j == LAG)
        def _():
            with jax.named_scope("a1_7"):
                a_local(1).wait()
                a_part(1).wait_recv()
                for half in range(2):
                    a_third(1, half)
                    a_fourth(1, half)

        @pl.when(j == last - 3)
        def _():
            with jax.named_scope("sum_last"):
                sum_last()

        @pl.when(j == last)
        def _():
            with jax.named_scope("drain"):
                drain()

        @pl.when(j == last + 1)
        def _():
            with jax.named_scope("merge_last"):
                merge_last()

        def own(i, inner):
            buf = lax.rem(i, 2)
            r_load(i).start()
            with jax.named_scope("local_load_wait"):
                for k in range(4):
                    w_load(buf, i, k).wait()
            with jax.named_scope("gemm1"):
                gemm_own(buf)

            @pl.when((buf == 1) & (i + 2 < last))
            def _():
                w_loads(1, i + 2)

            r_load(i).wait()
            with jax.named_scope("o_recv_wait"):
                out_copy(i).wait_recv()
            with jax.named_scope("merge"):
                for_rows(lambda rs: finish(i, rs, wide(rv[rs, :]) + (lv[rs, :] + hbuf[i, rs, :])))
            return inner

        @pl.when(j >= LAG)
        def _():
            n = 2 * (j - LAG)
            lax.fori_loop(jnp.maximum(n - 1, 0), jnp.minimum(n + 1, last), own, 0)

        @pl.when(j == last - 3)
        def _():
            sf_copy().start()

        return carry

    def drain():
        def sent(ref, sem):
            remote(ref, ref, sem, sf_recv, part).wait_send()

        sent(wbuf.at[1], wa_send)
        sent(wbuf.at[0], wp_send)
        sent(wbuf.at[2], wf_send)
        sent(av.at[0, pl.ds(0, 2)], ap_send)
        sent(av.at[0, 0], ax_send)
        sent(av.at[0, pl.ds(0, 2)], ay_send)
        sent(av.at[0, 0], af_send)
        sent(sb, sb_send)
        sent(sp, sp_send)

    lax.fori_loop(0, LAG + (last + 1) // 2, step, 0)

    with jax.named_scope("sums"):
        svr[y] = lax.dot_general(jnp.ones((8, 128), jnp.float32), ssacc[...], (((1,), (1,)), ((), ())),
                                 preferred_element_type=jnp.float32, precision=lax.Precision.HIGHEST)
        sf_copy().wait_send()
        out_copy(last - 2).wait_send()
        out_copy(last - 1).wait_send()
    with jax.named_scope("sums_exchange"):
        sums = [remote(svr.at[y], svr.at[y], s_send, s_recv.at[d - 1], {"tp2": lax.rem(y + d, ny)})
                for d in range(1, ny)]
        for copy in sums:
            copy.start()
        for d in range(1, ny):
            src = lax.rem(y + ny - d, ny)
            remote(svr.at[src], svr.at[src], s_send, s_recv.at[d - 1], part).wait_recv()
        total = svr[0]
        for q in range(1, ny):
            total = total + svr[q]
        ssq_out[...] = total
        ref = svr.at[pl.ds(0, ny - 1)]
        remote(ref, ref, s_send, s_recv.at[0], part).wait_send()


def norm_kernel(width, h, ssq, gain, hidden, normed, scale, hs, ns, h_sem, n_sem):
    chunks, rows, cols = h.shape
    span = 64
    inv_rms = lax.rsqrt(ssq[...] / width + EPS_NORM)
    scale[...] = jnp.broadcast_to(jnp.transpose(inv_rms)[:, :1], scale.shape)

    def block(t, carry):
        rs = pl.ds(pl.multiple_of(t * span, span), span)
        factor = scale[rs, :]
        for j in range(chunks):
            cs = slice(j * cols, (j + 1) * cols)
            value = h[j, rs, :]
            hs[rs, cs] = value.astype(jnp.bfloat16)
            ns[rs, cs] = (value * factor * gain[:, cs]).astype(jnp.bfloat16)
        pltpu.make_async_copy(hs.at[rs], hidden.at[rs], h_sem).start()
        pltpu.make_async_copy(ns.at[rs], normed.at[rs], n_sem).start()
        return carry

    lax.fori_loop(0, rows // span, block, 0)
    pltpu.make_async_copy(hs, hidden, h_sem).wait()
    pltpu.make_async_copy(ns, normed, n_sem).wait()


def solution(mesh):
    tp, ny = mesh.shape["tp"], mesh.shape["tp2"]
    chips = tp // CORES

    def local_step(a, w, r, gain):
        depth, cols = w.shape
        rows = r.shape[0]
        last = cols // CN - 1
        dma = pltpu.SemaphoreType.DMA
        any_space = pl.BlockSpec(memory_space=pl.ANY)
        bf16, f32 = jnp.bfloat16, jnp.float32
        chunks = last + 1
        vmem = pl.BlockSpec(memory_space=pltpu.VMEM)
        h, ssq, _ = pl.pallas_call(
            functools.partial(kernel, ny, chips),
            out_shape=(
                pltpu.VMEM((chunks, rows, CN), f32),
                pltpu.VMEM((8, rows), f32),
                jax.ShapeDtypeStruct((3, last, depth, CN), bf16),
            ),
            in_specs=[any_space] * 3,
            out_specs=(vmem, vmem, any_space),
            scratch_shapes=[
                pltpu.VMEM((2, 4, rows, depth), bf16),
                pltpu.VMEM((2, 4, depth, CN), bf16),
                pltpu.VMEM((2, rows, CN), f32),
                pltpu.VMEM((rows, CN), f32),
                pltpu.VMEM((rows, CN), bf16),
                pltpu.VMEM((rows, 128), f32),
                pltpu.VMEM((ny, 8, rows), f32),
                pltpu.VMEM((2, rows, depth), bf16),
                pltpu.VMEM((8, rows, CN), bf16),
                pltpu.VMEM((4, rows, CN), bf16),
                pltpu.VMEM((2, rows, CN), bf16),
                pltpu.VMEM((rows, CN), f32),
                dma((2,)), dma(()), dma((2,)), dma(()), dma((2, 2, PIECES)),
                dma(()), dma((2, 2, PIECES)), dma((2, 2)), dma(()), dma((2, 2)),
                dma(()), dma((last,)), dma(()), dma((last,)), dma(()), dma((last,)),
                dma((2,)), dma((last,)),
                dma((2, 4)), dma(()), dma(()), dma((ny - 1,)),
                dma((2,)), dma(()), dma((4,)), dma(()), dma((2,)), dma(()), dma(()),
            ],
            compiler_params=pltpu.CompilerParams(
                collective_id=0, has_side_effects=True, vmem_limit_bytes=54400000),
            cost_estimate=pl.CostEstimate(
                flops=2 * 8 * rows * depth * cols, bytes_accessed=8 * depth * cols * 2, transcendentals=0),
        )(a, w, r)
        return pl.pallas_call(
            functools.partial(norm_kernel, cols * ny),
            out_shape=(jax.ShapeDtypeStruct((rows, cols), bf16),) * 2,
            in_specs=[vmem] * 3,
            out_specs=(any_space, any_space),
            scratch_shapes=[
                pltpu.VMEM((rows, CN), f32), pltpu.VMEM((rows, cols), bf16), pltpu.VMEM((rows, cols), bf16),
                dma(()), dma(()),
            ],
            compiler_params=pltpu.CompilerParams(vmem_limit_bytes=24 << 20),
            cost_estimate=pl.CostEstimate(flops=4 * rows * cols, bytes_accessed=8 * rows * cols, transcendentals=rows),
        )(pltpu.with_memory_space_constraint(h, pltpu.VMEM), pltpu.with_memory_space_constraint(ssq, pltpu.VMEM), gain.reshape(1, cols))

    row_spec = P(("dp", "tp"), "tp2")
    return jax.shard_map(local_step, mesh=mesh, in_specs=(P("dp", "tp"), P("tp", "tp2"), row_spec, P("tp2")),
                         out_specs=(row_spec, row_spec), check_vma=False)
```

```python
import functools

import jax
import jax.numpy as jnp
from jax import lax
from jax.experimental import pallas as pl
from jax.experimental.pallas import tpu as pltpu
from jax.sharding import PartitionSpec as P

EPS_NORM = 1e-6
MESH = pl.DeviceIdType.MESH
CORES = 2
CN = 256
LAG = 7
AHEAD = 7
PIECES = 4


def kernel(ny, chips, a, w, r, hbuf, ssq_out, wbuf, av, wv, ov, lv, rv, ssacc, svr, at, pv, sb, sp, sg,
           al_sem, ap_send, ap_recv, ax_send, ax_recv, ay_send, ay_recv, ao_recv, af_send, af_recv,
           wp_send, wp_recv, wa_send, wa_recv, wf_send, wf_recv, o_send, o_recv,
           wl_sem, r_sem, s_send, s_recv, at_sem, sb_send, sb_recv, sp_send, sp_recv, sf_send, sf_recv):
    rows, cols = r.shape
    last = cols // CN - 1
    quarter = rows // ny
    piece = quarter // PIECES
    tile = min(256, rows)
    me, y = lax.axis_index("tp"), lax.axis_index("tp2")
    x, c = lax.div(me, CORES), lax.rem(me, CORES)
    o = 1 - c
    xa = x + 1 - 2 * lax.rem(x, 2)
    xb = chips - 1 - x
    xab = chips - 1 - xa
    yp, ym = lax.rem(y + 1, ny), lax.rem(y + ny - 1, ny)
    part = {"tp": x * CORES + o}
    acore, aother = {"tp": xa * CORES + c}, {"tp": xa * CORES + o}
    bcore, bother = {"tp": xb * CORES + c}, {"tp": xb * CORES + o}
    up, down = {"tp2": yp}, {"tp2": ym}

    def remote(src, dst, send, recv, device):
        return pltpu.make_async_remote_copy(
            src_ref=src, dst_ref=dst, send_sem=send, recv_sem=recv, device_id=device, device_id_type=MESH)

    def arow(owner, size=None, shift=0):
        return pl.ds(pl.multiple_of(owner * rows + shift, 16), rows if size is None else size)

    def qrow(q, t):
        return pl.ds(pl.multiple_of(q * quarter + t * piece, 16), piece)

    def wcol(j):
        return pl.ds(pl.multiple_of(j * CN, CN), CN)

    own_rows = (xb * CORES + c, me)
    part_rows = (xb * CORES + o, x * CORES + o)

    def a_local(g):
        return pltpu.make_async_copy(a.at[arow(own_rows[g])], av.at[g, 0], al_sem.at[g])

    def a_part(g):
        return remote(a.at[arow(part_rows[g])], av.at[g, 1], ap_send, ap_recv.at[g], part)

    def a_cross(g, s, t):
        core, device = ((c, acore), (o, aother))[s]
        owner = (xab, xa)[g] * CORES + core
        return remote(a.at[arow(owner, piece, y * quarter + t * piece)], av.at[g, 2 + s, qrow(y, t)],
                      ax_send, ax_recv.at[g, s, t], device)

    def a_near(g, s, t, d):
        ref = av.at[g, 2 + s, qrow(y, t)]
        recv = ay_recv.at[g, s, t] if d == s else ao_recv.at[g, t // (PIECES // 2)]
        return remote(ref, ref, ay_send, recv, (up, down)[d])

    def a_far(g, s, t):
        ref = av.at[g, 2 + s, qrow((ym, yp)[s], t)]
        return remote(ref, ref, af_send, af_recv.at[g, t // (PIECES // 2)], (up, down)[s])

    halves = (range(PIECES // 2), range(PIECES // 2, PIECES))

    def a_first(g, s, t):
        a_cross(g, s, t).wait_recv()
        for d in range(2):
            a_near(g, s, t, d).start()

    def a_second(g, s, t):
        a_near(g, s, t, s).wait_recv()
        a_far(g, s, t).start()

    def half_arrival(sem, g):
        ref = av.at[g, 2, pl.ds(0, quarter)]
        return remote(ref, ref, ay_send, sem, part)

    def a_third(g, half):
        half_arrival(ao_recv.at[g, half], g).wait_recv()

    def a_fourth(g, half):
        half_arrival(af_recv.at[g, half], g).wait_recv()

    def w_part(j):
        return remote(w.at[:, wcol(j)], wbuf.at[0, j], wp_send, wp_recv.at[j], part)

    def w_cross(j):
        return remote(w.at[:, wcol(j)], wbuf.at[1, j], wa_send, wa_recv.at[j], acore)

    def w_pass(j):
        return remote(wbuf.at[1, j], wbuf.at[2, j], wf_send, wf_recv.at[j], part)

    def w_load(g, j, k):
        src = w.at[:, wcol(j)] if k == 0 else wbuf.at[k - 1, j]
        return pltpu.make_async_copy(src, wv.at[g, k], wl_sem.at[g, k])

    def w_loads(g, j):
        for k in range(4):
            w_load(g, j, k).start()

    def out_copy(j):
        slot = lax.rem(j, 2)
        return remote(ov.at[slot], hbuf.at[j], o_send.at[slot], o_recv.at[j], bcore)

    def out_rows(i):
        half, k = lax.div(i, ny), lax.rem(i, ny)
        shift = lax.div(k + 1, 2) * (2 * lax.rem(k, 2) - 1)
        q = lax.rem(y + shift + ny, ny)
        return pl.ds(pl.multiple_of(q * quarter + half * (quarter // 2), 16), quarter // 2)

    def out_part(j, i):
        slot, rs = lax.rem(j, 2), out_rows(i)
        return remote(ov.at[slot, rs], hbuf.at[j, rs], o_send.at[slot], o_recv.at[j], bcore)

    def r_load(j):
        return pltpu.make_async_copy(r.at[:, wcol(j)], rv, r_sem)

    def block_product(lhs, rhs):
        return jnp.dot(lhs, rhs, preferred_element_type=jnp.float32).astype(jnp.bfloat16)

    def summed(g, buf, rs):
        acc = None
        for k in range(4):
            prod = block_product(av[g, k, rs, :], wv[buf, k]).astype(jnp.float32)
            acc = prod if acc is None else acc + prod
        return acc

    def gemm_out(j):
        slot = lax.rem(j, 2)
        late = (j <= 1) | (j == 4) | (j == LAG)

        def step(i, carry):
            @pl.when((j == 0) & (i == ny - 1))
            def _():
                a_fourth(0, 0)

            @pl.when((j == 0) & (i == ny))
            def _():
                with jax.named_scope("a0_half"):
                    for t in halves[1]:
                        for s in range(2):
                            a_first(0, s, t)
                    for t in halves[1]:
                        for s in range(2):
                            a_second(0, s, t)
                    a_third(0, 1)

            @pl.when((j == 0) & (i == 2 * ny - 1))
            def _():
                with jax.named_scope("a0_far"):
                    a_fourth(0, 1)

            rs = out_rows(i)
            ov[slot, rs, :] = summed(0, 0, rs)

            @pl.when((i >= 1) & late)
            def _():
                out_part(j, i - 1).start()

            return carry

        lax.fori_loop(0, 2 * ny, step, 0)

    def gemm_own(buf):
        def step(i, carry):
            rs = pl.ds(pl.multiple_of(i * tile, tile), tile)
            lv[rs, :] = summed(1, buf, rs)
            return carry

        lax.fori_loop(0, rows // tile, step, 0)

    items = ((xb, 0), (xb, 1), (xab, 0), (xab, 1), (x, o), (xa, o), (x, c), (xa, c))

    def at_load(n):
        pos, core = items[n]
        return pltpu.make_async_copy(a.at[arow(pos * CORES + core)], at.at[n % 2], at_sem.at[n % 2])

    def item_send(n):
        if n < 4:
            slot = n // 2 * 2 + c
            device = {"tp": xb * CORES + n % 2}
            return remote(pv.at[n], sb.at[slot], sb_send, sb_recv.at[slot], device)
        return remote(pv.at[n], sp.at[n - 4], sp_send, sp_recv.at[n - 4], part)

    def item(n):
        at_load(n).wait()

        def step(i, carry):
            rs = pl.ds(pl.multiple_of(i * tile, tile), tile)
            pv[n, rs, :] = block_product(at[n % 2, rs, :], wv[0, 0])
            return carry

        lax.fori_loop(0, rows // tile, step, 0)
        if n + 2 < len(items):
            at_load(n + 2).start()

    def sb_arrival(slot):
        return remote(pv.at[0], sb.at[slot], sb_send, sb_recv.at[slot], bcore)

    def sf_copy():
        return remote(sg, hbuf.at[last], sf_send, sf_recv, acore)

    def for_rows(body):
        def step(t, carry):
            body(pl.ds(pl.multiple_of(t * 64, 64), 64))
            return carry

        lax.fori_loop(0, rows // 64, step, 0)

    def finish(j, rs, h):
        hbuf[j, rs, :] = h
        sq = h * h
        acc = ssacc[rs, :]
        for l in range(CN // 128):
            acc = acc + sq[:, l * 128:(l + 1) * 128]
        ssacc[rs, :] = acc

    def wide(v):
        return v.astype(jnp.float32)

    barrier = pltpu.get_barrier_semaphore()
    peers = [part, acore, aother, bcore, bother] + [{"tp2": lax.rem(y + d, ny)} for d in range(1, ny)]
    for peer in peers:
        pl.semaphore_signal(barrier, inc=1, device_id=peer, device_id_type=MESH)
    w_last = pltpu.make_async_copy(w.at[:, wcol(last)], wv.at[0, 0], wl_sem.at[0, 0])
    w_last.start()
    at_load(0).start()
    at_load(1).start()
    pl.semaphore_wait(barrier, len(peers))

    for t in halves[0]:
        for s in range(2):
            a_cross(0, s, t).start()
    a_part(0).start()
    for j in range(AHEAD):
        w_cross(j).start()
        w_part(j).start()
        if j == 0:
            for t in halves[1]:
                for s in range(2):
                    a_cross(0, s, t).start()
        if j in (3, 6):
            for t in range(PIECES):
                a_cross(1, j // 6, t).start()
    a_part(1).start()
    w_last.wait()
    with jax.named_scope("items"):
        item(0)
        item(1)
        item_send(0).start()
        item(2)
        item_send(1).start()
        item(3)
        item_send(2).start()
    a_local(0).start()
    a_local(1).start()
    ssacc[...] = jnp.zeros_like(ssacc)
    item_send(3).start()
    with jax.named_scope("a0_first"):
        for t in halves[0]:
            for s in range(2):
                a_first(0, s, t)
    with jax.named_scope("items_2"):
        for n in range(4, 8):
            item(n)
        item_send(4).start()
        item_send(5).start()
    with jax.named_scope("a0_second"):
        for t in halves[0]:
            for s in range(2):
                a_second(0, s, t)
    with jax.named_scope("a0_third"):
        a_local(0).wait()
        a_part(0).wait_recv()
        a_third(0, 0)

    def merge_last():
        r_load(last).start()
        sb_arrival(0).wait_recv()
        sb_arrival(1).wait_recv()
        with jax.named_scope("sf_wait"):
            sf_copy().wait_recv()
        r_load(last).wait()
        for_rows(lambda rs: finish(last, rs, wide(rv[rs, :]) + (
            (wide(pv[6, rs, :]) + wide(sp[0, rs, :])) + (wide(sb[0, rs, :]) + wide(sb[1, rs, :])) + hbuf[last, rs, :])))

    def sum_last():
        for n in range(2):
            item_send(4 + n).wait_recv()
            sb_arrival(2 + n).wait_recv()

        def body(rs):
            sg[rs, :] = (wide(pv[7, rs, :]) + wide(sp[1, rs, :])) + (wide(sb[2, rs, :]) + wide(sb[3, rs, :]))

        for_rows(body)

    def step(j, carry):
        @pl.when(j < last)
        def _():
            with jax.named_scope("w_cross_wait"):
                w_cross(j).wait_recv()
            w_pass(j).start()

            @pl.when(j + AHEAD < last)
            def _():
                w_cross(j + AHEAD).start()
                w_part(j + AHEAD).start()

            w_load(0, j, 0).start()
            w_load(0, j, 2).start()
            with jax.named_scope("w_pass_wait"):
                w_part(j).wait_recv()
                w_load(0, j, 1).start()
                w_pass(j).wait_recv()
                w_load(0, j, 3).start()

            @pl.when(j >= 2)
            def _():
                with jax.named_scope("o_send_wait"):
                    out_copy(j - 2).wait_send()

            with jax.named_scope("w_load_wait"):
                for k in range(4):
                    w_load(0, j, k).wait()
            with jax.named_scope("gemm0"):
                gemm_out(j)

            late = (j <= 1) | (j == 4) | (j == LAG)

            @pl.when(late)
            def _():
                out_part(j, 2 * ny - 1).start()

            @pl.when(jnp.logical_not(late))
            def _():
                out_copy(j).start()

        @pl.when(j == LAG)
        def _():
            w_loads(1, 1)

        @pl.when((j >= LAG) & (2 * (j - LAG) < last))
        def _():
            w_loads(0, 2 * (j - LAG))

        @pl.when(j == 3)
        def _():
            with jax.named_scope("a1_3"):
                for t in range(PIECES):
                    a_first(1, 0, t)

        @pl.when(j == 4)
        def _():
            with jax.named_scope("a1_4"):
                for t in range(PIECES):
                    a_second(1, 0, t)

        @pl.when(j == LAG - 1)
        def _():
            with jax.named_scope("a1_6"):
                for t in range(PIECES):
                    a_first(1, 1, t)
                for t in range(PIECES):
                    a_second(1, 1, t)

        @pl.when(j == LAG)
        def _():
            with jax.named_scope("a1_7"):
                a_local(1).wait()
                a_part(1).wait_recv()
                for half in range(2):
                    a_third(1, half)
                    a_fourth(1, half)

        @pl.when(j == last - 3)
        def _():
            with jax.named_scope("sum_last"):
                sum_last()

        @pl.when(j == last)
        def _():
            with jax.named_scope("drain"):
                drain()

        @pl.when(j == last + 1)
        def _():
            with jax.named_scope("merge_last"):
                merge_last()

        def own(i, inner):
            buf = lax.rem(i, 2)
            r_load(i).start()
            with jax.named_scope("local_load_wait"):
                for k in range(4):
                    w_load(buf, i, k).wait()
            with jax.named_scope("gemm1"):
                gemm_own(buf)

            @pl.when((buf == 1) & (i + 2 < last))
            def _():
                w_loads(1, i + 2)

            r_load(i).wait()
            with jax.named_scope("o_recv_wait"):
                out_copy(i).wait_recv()
            with jax.named_scope("merge"):
                for_rows(lambda rs: finish(i, rs, wide(rv[rs, :]) + (lv[rs, :] + hbuf[i, rs, :])))
            return inner

        @pl.when(j >= LAG)
        def _():
            n = 2 * (j - LAG)
            lax.fori_loop(jnp.maximum(n - 1, 0), jnp.minimum(n + 1, last), own, 0)

        @pl.when(j == last - 3)
        def _():
            sf_copy().start()

        return carry

    def drain():
        def sent(ref, sem):
            remote(ref, ref, sem, sf_recv, part).wait_send()

        sent(wbuf.at[1], wa_send)
        sent(wbuf.at[0], wp_send)
        sent(wbuf.at[2], wf_send)
        sent(av.at[0, pl.ds(0, 2)], ap_send)
        sent(av.at[0, 0], ax_send)
        sent(av.at[0, pl.ds(0, 2)], ay_send)
        sent(av.at[0, 0], af_send)
        sent(sb, sb_send)
        sent(sp, sp_send)

    lax.fori_loop(0, LAG + (last + 1) // 2, step, 0)

    with jax.named_scope("sums"):
        full = lax.dot_general(jnp.ones((8, 128), jnp.float32), ssacc[...], (((1,), (1,)), ((), ())),
                               preferred_element_type=jnp.float32, precision=lax.Precision.HIGHEST)
        line = lax.broadcasted_iota(jnp.int32, (8, 128), 0)
        packed = jnp.zeros((8, 128), jnp.float32)
        for b in range(rows // 128):
            packed = jnp.where(line == b, full[:, b * 128:(b + 1) * 128], packed)
        svr[y] = packed
        sf_copy().wait_send()
        out_copy(last - 2).wait_send()
        out_copy(last - 1).wait_send()
    with jax.named_scope("sums_exchange"):
        sums = [remote(svr.at[y], svr.at[y], s_send, s_recv.at[d - 1], {"tp2": lax.rem(y + d, ny)})
                for d in range(1, ny)]
        for copy in sums:
            copy.start()
        for d in range(1, ny):
            src = lax.rem(y + ny - d, ny)
            remote(svr.at[src], svr.at[src], s_send, s_recv.at[d - 1], part).wait_recv()
        total = svr[0]
        for q in range(1, ny):
            total = total + svr[q]
        ssq_out[...] = total
        ref = svr.at[pl.ds(0, ny - 1)]
        remote(ref, ref, s_send, s_recv.at[0], part).wait_send()


def norm_kernel(width, h, ssq, gain, hidden, normed, scale, hs, ns, h_sem, n_sem):
    chunks, rows, cols = h.shape
    span = 64
    inv_rms = lax.rsqrt(ssq[...] / width + EPS_NORM)
    columns = jnp.transpose(inv_rms)
    for b in range(rows // 128):
        scale[b * 128:(b + 1) * 128, :] = jnp.broadcast_to(columns[:, b:b + 1], (128, scale.shape[1]))

    def block(t, carry):
        rs = pl.ds(pl.multiple_of(t * span, span), span)
        factor = scale[rs, :]
        for j in range(chunks):
            cs = slice(j * cols, (j + 1) * cols)
            value = h[j, rs, :]
            hs[rs, cs] = value.astype(jnp.bfloat16)
            ns[rs, cs] = (value * factor * gain[:, cs]).astype(jnp.bfloat16)
        pltpu.make_async_copy(hs.at[rs], hidden.at[rs], h_sem).start()
        pltpu.make_async_copy(ns.at[rs], normed.at[rs], n_sem).start()
        return carry

    lax.fori_loop(0, rows // span, block, 0)
    pltpu.make_async_copy(hs, hidden, h_sem).wait()
    pltpu.make_async_copy(ns, normed, n_sem).wait()


def solution(mesh):
    tp, ny = mesh.shape["tp"], mesh.shape["tp2"]
    chips = tp // CORES

    def local_step(a, w, r, gain):
        depth, cols = w.shape
        rows = r.shape[0]
        last = cols // CN - 1
        dma = pltpu.SemaphoreType.DMA
        any_space = pl.BlockSpec(memory_space=pl.ANY)
        bf16, f32 = jnp.bfloat16, jnp.float32
        chunks = last + 1
        vmem = pl.BlockSpec(memory_space=pltpu.VMEM)
        h, ssq, _ = pl.pallas_call(
            functools.partial(kernel, ny, chips),
            out_shape=(
                pltpu.VMEM((chunks, rows, CN), f32),
                pltpu.VMEM((8, 128), f32),
                jax.ShapeDtypeStruct((3, last, depth, CN), bf16),
            ),
            in_specs=[any_space] * 3,
            out_specs=(vmem, vmem, any_space),
            scratch_shapes=[
                pltpu.VMEM((2, 4, rows, depth), bf16),
                pltpu.VMEM((2, 4, depth, CN), bf16),
                pltpu.VMEM((2, rows, CN), f32),
                pltpu.VMEM((rows, CN), f32),
                pltpu.VMEM((rows, CN), bf16),
                pltpu.VMEM((rows, 128), f32),
                pltpu.VMEM((ny, 8, 128), f32),
                pltpu.VMEM((2, rows, depth), bf16),
                pltpu.VMEM((8, rows, CN), bf16),
                pltpu.VMEM((4, rows, CN), bf16),
                pltpu.VMEM((2, rows, CN), bf16),
                pltpu.VMEM((rows, CN), f32),
                dma((2,)), dma(()), dma((2,)), dma(()), dma((2, 2, PIECES)),
                dma(()), dma((2, 2, PIECES)), dma((2, 2)), dma(()), dma((2, 2)),
                dma(()), dma((last,)), dma(()), dma((last,)), dma(()), dma((last,)),
                dma((2,)), dma((last,)),
                dma((2, 4)), dma(()), dma(()), dma((ny - 1,)),
                dma((2,)), dma(()), dma((4,)), dma(()), dma((2,)), dma(()), dma(()),
            ],
            compiler_params=pltpu.CompilerParams(
                collective_id=0, has_side_effects=True, vmem_limit_bytes=54400000),
            cost_estimate=pl.CostEstimate(
                flops=2 * 8 * rows * depth * cols, bytes_accessed=8 * depth * cols * 2, transcendentals=0),
        )(a, w, r)
        return pl.pallas_call(
            functools.partial(norm_kernel, cols * ny),
            out_shape=(jax.ShapeDtypeStruct((rows, cols), bf16),) * 2,
            in_specs=[vmem] * 3,
            out_specs=(any_space, any_space),
            scratch_shapes=[
                pltpu.VMEM((rows, CN), f32), pltpu.VMEM((rows, cols), bf16), pltpu.VMEM((rows, cols), bf16),
                dma(()), dma(()),
            ],
            compiler_params=pltpu.CompilerParams(vmem_limit_bytes=24 << 20),
            cost_estimate=pl.CostEstimate(flops=4 * rows * cols, bytes_accessed=8 * rows * cols, transcendentals=rows),
        )(pltpu.with_memory_space_constraint(h, pltpu.VMEM), pltpu.with_memory_space_constraint(ssq, pltpu.VMEM), gain.reshape(1, cols))

    row_spec = P(("dp", "tp"), "tp2")
    return jax.shard_map(local_step, mesh=mesh, in_specs=(P("dp", "tp"), P("tp", "tp2"), row_spec, P("tp2")),
                         out_specs=(row_spec, row_spec), check_vma=False)
```

```python
import functools

import jax
import jax.numpy as jnp
from jax import lax
from jax.experimental import pallas as pl
from jax.experimental.pallas import tpu as pltpu
from jax.sharding import PartitionSpec as P

EPS_NORM = 1e-6
MESH = pl.DeviceIdType.MESH
CORES = 2
CN = 256
LAG = 7
FIRST = 8
AHEAD = 6
PIECES = 4


def kernel(ny, chips, a, w, r, hbuf, ssq_out, wbuf, av, wv, ov, lv, rv, ssacc, svr, at, pv, sb, sp, sg,
           al_sem, ap_send, ap_recv, ax_send, ax_recv, ay_send, ay_recv, ao_recv, af_send, af_recv,
           wp_send, wp_recv, wa_send, wa_recv, wf_send, wf_recv, o_send, o_recv,
           wl_sem, r_sem, s_send, s_recv, at_sem, sb_send, sb_recv, sp_send, sp_recv, sf_send, sf_recv):
    rows, cols = r.shape
    last = cols // CN - 1
    quarter = rows // ny
    piece = quarter // PIECES
    tile = min(256, rows)
    me, y = lax.axis_index("tp"), lax.axis_index("tp2")
    x, c = lax.div(me, CORES), lax.rem(me, CORES)
    o = 1 - c
    xa = x + 1 - 2 * lax.rem(x, 2)
    xb = chips - 1 - x
    xab = chips - 1 - xa
    yp, ym = lax.rem(y + 1, ny), lax.rem(y + ny - 1, ny)
    part = {"tp": x * CORES + o}
    acore, aother = {"tp": xa * CORES + c}, {"tp": xa * CORES + o}
    bcore, bother = {"tp": xb * CORES + c}, {"tp": xb * CORES + o}
    up, down = {"tp2": yp}, {"tp2": ym}

    def remote(src, dst, send, recv, device):
        return pltpu.make_async_remote_copy(
            src_ref=src, dst_ref=dst, send_sem=send, recv_sem=recv, device_id=device, device_id_type=MESH)

    def arow(owner, size=None, shift=0):
        return pl.ds(pl.multiple_of(owner * rows + shift, 16), rows if size is None else size)

    def qrow(q, t):
        return pl.ds(pl.multiple_of(q * quarter + t * piece, 16), piece)

    def wcol(j):
        return pl.ds(pl.multiple_of(j * CN, CN), CN)

    own_rows = (xb * CORES + c, me)
    part_rows = (xb * CORES + o, x * CORES + o)

    def a_local(g):
        return pltpu.make_async_copy(a.at[arow(own_rows[g])], av.at[g, 0], al_sem.at[g])

    def a_part(g):
        return remote(a.at[arow(part_rows[g])], av.at[g, 1], ap_send, ap_recv.at[g], part)

    def a_cross(g, s, t):
        core, device = ((c, acore), (o, aother))[s]
        owner = (xab, xa)[g] * CORES + core
        return remote(a.at[arow(owner, piece, y * quarter + t * piece)], av.at[g, 2 + s, qrow(y, t)],
                      ax_send, ax_recv.at[g, s, t], device)

    def a_near(g, s, t, d):
        ref = av.at[g, 2 + s, qrow(y, t)]
        recv = ay_recv.at[g, s, t] if d == s else ao_recv.at[g, max(t - 1, 0)]
        return remote(ref, ref, ay_send, recv, (up, down)[d])

    def a_far(g, s, t):
        ref = av.at[g, 2 + s, qrow((ym, yp)[s], t)]
        return remote(ref, ref, af_send, af_recv.at[g, max(t - 1, 0)], (up, down)[s])

    def a_first(g, s, t):
        a_cross(g, s, t).wait_recv()
        for d in range(2):
            a_near(g, s, t, d).start()

    def a_second(g, s, t):
        a_near(g, s, t, s).wait_recv()
        a_far(g, s, t).start()

    def group_arrival(sem, g, group):
        ref = av.at[g, 2, pl.ds(0, 2 * piece * (2 if group == 0 else 1))]
        return remote(ref, ref, ay_send, sem.at[g, group], part)

    def a_third(g, group):
        group_arrival(ao_recv, g, group).wait_recv()

    def a_fourth(g, group):
        group_arrival(af_recv, g, group).wait_recv()

    def w_part(j):
        return remote(w.at[:, wcol(j)], wbuf.at[0, j], wp_send, wp_recv.at[j], part)

    def w_cross(j):
        return remote(w.at[:, wcol(j)], wbuf.at[1, j], wa_send, wa_recv.at[j], acore)

    def w_pass(j):
        return remote(wbuf.at[1, j], wbuf.at[2, j], wf_send, wf_recv.at[j], part)

    def w_load(g, j, k):
        src = w.at[:, wcol(j)] if k == 0 else wbuf.at[k - 1, j]
        return pltpu.make_async_copy(src, wv.at[g, k], wl_sem.at[g, k])

    def w_loads(g, j):
        for k in range(4):
            w_load(g, j, k).start()

    def out_copy(j):
        slot = lax.rem(j, 2)
        return remote(ov.at[slot], hbuf.at[j], o_send.at[slot], o_recv.at[j], bcore)

    def quarter_of(k):
        return lax.rem(y + lax.div(k + 1, 2) * (2 * lax.rem(k, 2) - 1) + ny, ny)

    def out_rows(i):
        return pl.ds(pl.multiple_of(quarter_of(i) * quarter, 16), quarter)

    def out_part(j, rs):
        slot = lax.rem(j, 2)
        return remote(ov.at[slot, rs], hbuf.at[j, rs], o_send.at[slot], o_recv.at[j], bcore)

    def r_load(j):
        return pltpu.make_async_copy(r.at[:, wcol(j)], rv, r_sem)

    def block_product(lhs, rhs):
        return jnp.dot(lhs, rhs, preferred_element_type=jnp.float32).astype(jnp.bfloat16)

    def summed(g, buf, rs):
        acc = None
        for k in range(4):
            prod = block_product(av[g, k, rs, :], wv[buf, k]).astype(jnp.float32)
            acc = prod if acc is None else acc + prod
        return acc

    def in_parts(j):
        return (j == 2) | (j == 5) | (j == 8)

    def gemm_out(j):
        slot = lax.rem(j, 2)

        def step(i, carry):
            rs = out_rows(i)
            ov[slot, rs, :] = summed(0, 0, rs)

            @pl.when((i >= 1) & in_parts(j))
            def _():
                out_part(j, out_rows(i - 1)).start()

            return carry

        lax.fori_loop(0, ny, step, 0)

    def load_chunk(j, buf):
        with jax.named_scope("w_cross_wait"):
            w_cross(j).wait_recv()
        w_pass(j).start()
        w_load(buf, j, 0).start()
        w_load(buf, j, 2).start()
        with jax.named_scope("w_pass_wait"):
            w_part(j).wait_recv()
            w_load(buf, j, 1).start()
            w_pass(j).wait_recv()
            w_load(buf, j, 3).start()

    def load_wait(j, buf):
        with jax.named_scope("w_load_wait"):
            for k in range(4):
                w_load(buf, j, k).wait()

    most = (PIECES - 1) * ny

    def first_part(n):
        late = lax.div(n, 2 * most)
        early = 1 - late
        j = late * lax.rem(n, 2) + early * lax.div(n, most)
        t = late * (PIECES - 1) + early * lax.div(lax.rem(n, most), ny)
        k = late * lax.div(n - 2 * most, 2) + early * lax.rem(n, ny)
        return j, pl.ds(pl.multiple_of(quarter_of(k) * quarter + t * piece, 16), piece)

    def pass_on(t):
        for s in range(2):
            a_first(0, s, t)
        for s in range(2):
            a_second(0, s, t)
        a_third(0, t - 1)

    def first_chunks():
        def step(n, carry):
            @pl.when(n == ny - 1)
            def _():
                a_fourth(0, 0)

            @pl.when(n == 2 * ny)
            def _():
                with jax.named_scope("a0_piece2"):
                    pass_on(2)

            @pl.when(n == 3 * ny - 1)
            def _():
                with jax.named_scope("a0_far2"):
                    a_fourth(0, 1)

            @pl.when(n == most)
            def _():
                load_chunk(1, 1)
                load_wait(1, 1)

            @pl.when(n == 2 * most)
            def _():
                with jax.named_scope("a0_piece3"):
                    pass_on(3)

            @pl.when(n == 2 * most + 2 * ny - 2)
            def _():
                with jax.named_scope("a0_far3"):
                    a_fourth(0, 2)

            j, rs = first_part(n)
            ov[j, rs, :] = summed(0, j, rs)

            @pl.when(n >= 1)
            def _():
                out_part(*first_part(n - 1)).start()

            return carry

        lax.fori_loop(0, 2 * PIECES * ny, step, 0)
        out_part(*first_part(2 * PIECES * ny - 1)).start()

    def gemm_own(buf):
        def step(i, carry):
            rs = pl.ds(pl.multiple_of(i * tile, tile), tile)
            lv[rs, :] = summed(1, buf, rs)
            return carry

        lax.fori_loop(0, rows // tile, step, 0)

    items = ((xb, 0), (xb, 1), (xab, 0), (xab, 1), (x, o), (xa, o), (x, c), (xa, c))

    def at_load(n):
        pos, core = items[n]
        return pltpu.make_async_copy(a.at[arow(pos * CORES + core)], at.at[n % 2], at_sem.at[n % 2])

    def item_send(n):
        if n < 4:
            slot = n // 2 * 2 + c
            device = {"tp": xb * CORES + n % 2}
            return remote(pv.at[n], sb.at[slot], sb_send, sb_recv.at[slot], device)
        return remote(pv.at[n], sp.at[n - 4], sp_send, sp_recv.at[n - 4], part)

    def item(n):
        at_load(n).wait()

        def step(i, carry):
            rs = pl.ds(pl.multiple_of(i * tile, tile), tile)
            pv[n, rs, :] = block_product(at[n % 2, rs, :], wv[0, 0])
            return carry

        lax.fori_loop(0, rows // tile, step, 0)
        if n + 2 < len(items):
            at_load(n + 2).start()

    def sb_arrival(slot):
        return remote(pv.at[0], sb.at[slot], sb_send, sb_recv.at[slot], bcore)

    def sf_copy():
        return remote(sg, hbuf.at[last], sf_send, sf_recv, acore)

    def for_rows(body):
        def step(t, carry):
            body(pl.ds(pl.multiple_of(t * 64, 64), 64))
            return carry

        lax.fori_loop(0, rows // 64, step, 0)

    def finish(j, rs, h):
        hbuf[j, rs, :] = h
        sq = h * h
        acc = ssacc[rs, :]
        for l in range(CN // 128):
            acc = acc + sq[:, l * 128:(l + 1) * 128]
        ssacc[rs, :] = acc

    def wide(v):
        return v.astype(jnp.float32)

    barrier = pltpu.get_barrier_semaphore()
    peers = [part, acore, aother, bcore, bother] + [{"tp2": lax.rem(y + d, ny)} for d in range(1, ny)]
    for peer in peers:
        pl.semaphore_signal(barrier, inc=1, device_id=peer, device_id_type=MESH)
    w_last = pltpu.make_async_copy(w.at[:, wcol(last)], wv.at[0, 0], wl_sem.at[0, 0])
    w_last.start()
    at_load(0).start()
    at_load(1).start()
    pl.semaphore_wait(barrier, len(peers))

    for t in range(2):
        for s in range(2):
            a_cross(0, s, t).start()
    a_part(0).start()
    for j in range(FIRST):
        w_cross(j).start()
        w_part(j).start()
        if j < 2:
            for s in range(2):
                a_cross(0, s, j + 2).start()
        if j == 4:
            for t in range(PIECES):
                a_cross(1, 0, t).start()
        if j in (6, 7):
            for t in range(2):
                a_cross(1, 1, 2 * (j - 6) + t).start()
    a_part(1).start()
    w_last.wait()
    with jax.named_scope("items"):
        item(0)
        item(1)
        item_send(0).start()
        item(2)
        item_send(1).start()
        item(3)
        item_send(2).start()
    a_local(0).start()
    a_local(1).start()
    ssacc[...] = jnp.zeros_like(ssacc)
    item_send(3).start()
    with jax.named_scope("a0_first"):
        for t in range(2):
            for s in range(2):
                a_first(0, s, t)
    with jax.named_scope("items_2"):
        for n in range(4, 8):
            item(n)
        item_send(4).start()
        item_send(5).start()
    with jax.named_scope("a0_second"):
        for t in range(2):
            for s in range(2):
                a_second(0, s, t)
    with jax.named_scope("a0_third"):
        a_local(0).wait()
        a_part(0).wait_recv()
        a_third(0, 0)
    load_chunk(0, 0)
    load_wait(0, 0)
    with jax.named_scope("first_chunks"):
        first_chunks()

    def merge_last():
        r_load(last).start()
        sb_arrival(0).wait_recv()
        sb_arrival(1).wait_recv()
        with jax.named_scope("sf_wait"):
            sf_copy().wait_recv()
        r_load(last).wait()
        for_rows(lambda rs: finish(last, rs, wide(rv[rs, :]) + (
            (wide(pv[6, rs, :]) + wide(sp[0, rs, :])) + (wide(sb[0, rs, :]) + wide(sb[1, rs, :])) + hbuf[last, rs, :])))

    def sum_last():
        for n in range(2):
            item_send(4 + n).wait_recv()
            sb_arrival(2 + n).wait_recv()

        def body(rs):
            sg[rs, :] = (wide(pv[7, rs, :]) + wide(sp[1, rs, :])) + (wide(sb[2, rs, :]) + wide(sb[3, rs, :]))

        for_rows(body)

    def step(j, carry):
        @pl.when(j < last)
        def _():
            load_chunk(j, 0)

            @pl.when(j + AHEAD < last)
            def _():
                w_cross(j + AHEAD).start()
                w_part(j + AHEAD).start()

            with jax.named_scope("o_send_wait"):
                out_copy(j - 2).wait_send()
            load_wait(j, 0)
            with jax.named_scope("gemm0"):
                gemm_out(j)

            @pl.when(in_parts(j))
            def _():
                out_part(j, out_rows(ny - 1)).start()

            @pl.when(jnp.logical_not(in_parts(j)))
            def _():
                out_copy(j).start()

        @pl.when(j == LAG)
        def _():
            w_loads(1, 1)

        @pl.when((j >= LAG) & (2 * (j - LAG) < last))
        def _():
            w_loads(0, 2 * (j - LAG))

        @pl.when(j == 4)
        def _():
            with jax.named_scope("a1_4"):
                for t in range(PIECES):
                    a_first(1, 0, t)

        @pl.when(j == 5)
        def _():
            with jax.named_scope("a1_5"):
                for t in range(PIECES):
                    a_second(1, 0, t)

        @pl.when(j == LAG - 1)
        def _():
            with jax.named_scope("a1_6"):
                for t in range(2):
                    a_first(1, 1, t)
                for t in range(2):
                    a_second(1, 1, t)

        @pl.when(j == LAG)
        def _():
            with jax.named_scope("a1_7"):
                for t in range(2, PIECES):
                    a_first(1, 1, t)
                for t in range(2, PIECES):
                    a_second(1, 1, t)
                a_local(1).wait()
                a_part(1).wait_recv()
                for group in range(3):
                    a_third(1, group)
                    a_fourth(1, group)

        @pl.when(j == last - 3)
        def _():
            with jax.named_scope("sum_last"):
                sum_last()

        @pl.when(j == last)
        def _():
            with jax.named_scope("drain"):
                drain()

        @pl.when(j == last + 1)
        def _():
            with jax.named_scope("merge_last"):
                merge_last()

        def own(i, inner):
            buf = lax.rem(i, 2)
            r_load(i).start()
            with jax.named_scope("local_load_wait"):
                for k in range(4):
                    w_load(buf, i, k).wait()
            with jax.named_scope("gemm1"):
                gemm_own(buf)

            @pl.when((buf == 1) & (i + 2 < last))
            def _():
                w_loads(1, i + 2)

            r_load(i).wait()
            with jax.named_scope("o_recv_wait"):
                out_copy(i).wait_recv()
            with jax.named_scope("merge"):
                for_rows(lambda rs: finish(i, rs, wide(rv[rs, :]) + (lv[rs, :] + hbuf[i, rs, :])))
            return inner

        @pl.when(j >= LAG)
        def _():
            n = 2 * (j - LAG)
            lax.fori_loop(jnp.maximum(n - 1, 0), jnp.minimum(n + 1, last), own, 0)

        @pl.when(j == last - 3)
        def _():
            sf_copy().start()

        return carry

    def drain():
        def sent(ref, sem):
            remote(ref, ref, sem, sf_recv, part).wait_send()

        sent(wbuf.at[1], wa_send)
        sent(wbuf.at[0], wp_send)
        sent(wbuf.at[2], wf_send)
        sent(av.at[0, pl.ds(0, 2)], ap_send)
        sent(av.at[0, 0], ax_send)
        sent(av.at[0, pl.ds(0, 2)], ay_send)
        sent(av.at[0, 0], af_send)
        sent(sb, sb_send)
        sent(sp, sp_send)

    lax.fori_loop(2, LAG + (last + 1) // 2, step, 0)

    with jax.named_scope("sums"):
        full = lax.dot_general(jnp.ones((8, 128), jnp.float32), ssacc[...], (((1,), (1,)), ((), ())),
                               preferred_element_type=jnp.float32, precision=lax.Precision.HIGHEST)
        line = lax.broadcasted_iota(jnp.int32, (8, 128), 0)
        packed = jnp.zeros((8, 128), jnp.float32)
        for b in range(rows // 128):
            packed = jnp.where(line == b, full[:, b * 128:(b + 1) * 128], packed)
        svr[y] = packed
        sf_copy().wait_send()
        out_copy(last - 2).wait_send()
        out_copy(last - 1).wait_send()
    with jax.named_scope("sums_exchange"):
        sums = [remote(svr.at[y], svr.at[y], s_send, s_recv.at[d - 1], {"tp2": lax.rem(y + d, ny)})
                for d in range(1, ny)]
        for copy in sums:
            copy.start()
        for d in range(1, ny):
            src = lax.rem(y + ny - d, ny)
            remote(svr.at[src], svr.at[src], s_send, s_recv.at[d - 1], part).wait_recv()
        total = svr[0]
        for q in range(1, ny):
            total = total + svr[q]
        ssq_out[...] = total
        ref = svr.at[pl.ds(0, ny - 1)]
        remote(ref, ref, s_send, s_recv.at[0], part).wait_send()


def norm_kernel(width, h, ssq, gain, hidden, normed, scale, hs, ns, h_sem, n_sem):
    chunks, rows, cols = h.shape
    span = 64
    inv_rms = lax.rsqrt(ssq[...] / width + EPS_NORM)
    columns = jnp.transpose(inv_rms)
    for b in range(rows // 128):
        scale[b * 128:(b + 1) * 128, :] = jnp.broadcast_to(columns[:, b:b + 1], (128, scale.shape[1]))

    def block(t, carry):
        rs = pl.ds(pl.multiple_of(t * span, span), span)
        factor = scale[rs, :]
        for j in range(chunks):
            cs = slice(j * cols, (j + 1) * cols)
            value = h[j, rs, :]
            hs[rs, cs] = value.astype(jnp.bfloat16)
            ns[rs, cs] = (value * factor * gain[:, cs]).astype(jnp.bfloat16)
        pltpu.make_async_copy(hs.at[rs], hidden.at[rs], h_sem).start()
        pltpu.make_async_copy(ns.at[rs], normed.at[rs], n_sem).start()
        return carry

    lax.fori_loop(0, rows // span, block, 0)
    pltpu.make_async_copy(hs, hidden, h_sem).wait()
    pltpu.make_async_copy(ns, normed, n_sem).wait()


def solution(mesh):
    tp, ny = mesh.shape["tp"], mesh.shape["tp2"]
    chips = tp // CORES

    def local_step(a, w, r, gain):
        depth, cols = w.shape
        rows = r.shape[0]
        last = cols // CN - 1
        dma = pltpu.SemaphoreType.DMA
        any_space = pl.BlockSpec(memory_space=pl.ANY)
        bf16, f32 = jnp.bfloat16, jnp.float32
        chunks = last + 1
        vmem = pl.BlockSpec(memory_space=pltpu.VMEM)
        h, ssq, _ = pl.pallas_call(
            functools.partial(kernel, ny, chips),
            out_shape=(
                pltpu.VMEM((chunks, rows, CN), f32),
                pltpu.VMEM((8, 128), f32),
                jax.ShapeDtypeStruct((3, last, depth, CN), bf16),
            ),
            in_specs=[any_space] * 3,
            out_specs=(vmem, vmem, any_space),
            scratch_shapes=[
                pltpu.VMEM((2, 4, rows, depth), bf16),
                pltpu.VMEM((2, 4, depth, CN), bf16),
                pltpu.VMEM((2, rows, CN), f32),
                pltpu.VMEM((rows, CN), f32),
                pltpu.VMEM((rows, CN), bf16),
                pltpu.VMEM((rows, 128), f32),
                pltpu.VMEM((ny, 8, 128), f32),
                pltpu.VMEM((2, rows, depth), bf16),
                pltpu.VMEM((8, rows, CN), bf16),
                pltpu.VMEM((4, rows, CN), bf16),
                pltpu.VMEM((2, rows, CN), bf16),
                pltpu.VMEM((rows, CN), f32),
                dma((2,)), dma(()), dma((2,)), dma(()), dma((2, 2, PIECES)),
                dma(()), dma((2, 2, PIECES)), dma((2, 3)), dma(()), dma((2, 3)),
                dma(()), dma((last,)), dma(()), dma((last,)), dma(()), dma((last,)),
                dma((2,)), dma((last,)),
                dma((2, 4)), dma(()), dma(()), dma((ny - 1,)),
                dma((2,)), dma(()), dma((4,)), dma(()), dma((2,)), dma(()), dma(()),
            ],
            compiler_params=pltpu.CompilerParams(
                collective_id=0, has_side_effects=True, vmem_limit_bytes=54400000),
            cost_estimate=pl.CostEstimate(
                flops=2 * 8 * rows * depth * cols, bytes_accessed=8 * depth * cols * 2, transcendentals=0),
        )(a, w, r)
        return pl.pallas_call(
            functools.partial(norm_kernel, cols * ny),
            out_shape=(jax.ShapeDtypeStruct((rows, cols), bf16),) * 2,
            in_specs=[vmem] * 3,
            out_specs=(any_space, any_space),
            scratch_shapes=[
                pltpu.VMEM((rows, CN), f32), pltpu.VMEM((rows, cols), bf16), pltpu.VMEM((rows, cols), bf16),
                dma(()), dma(()),
            ],
            compiler_params=pltpu.CompilerParams(vmem_limit_bytes=24 << 20),
            cost_estimate=pl.CostEstimate(flops=4 * rows * cols, bytes_accessed=8 * rows * cols, transcendentals=rows),
        )(pltpu.with_memory_space_constraint(h, pltpu.VMEM), pltpu.with_memory_space_constraint(ssq, pltpu.VMEM), gain.reshape(1, cols))

    row_spec = P(("dp", "tp"), "tp2")
    return jax.shard_map(local_step, mesh=mesh, in_specs=(P("dp", "tp"), P("tp", "tp2"), row_spec, P("tp2")),
                         out_specs=(row_spec, row_spec), check_vma=False)
```

```python
import functools

import jax
import jax.numpy as jnp
from jax import lax
from jax.experimental import pallas as pl
from jax.experimental.pallas import tpu as pltpu
from jax.sharding import PartitionSpec as P

EPS_NORM = 1e-6
MESH = pl.DeviceIdType.MESH
CORES = 2
CN = 256
LAG = 7
FIRST = 8
AHEAD = 6
PIECES = 4


def kernel(ny, chips, a, w, r, hbuf, ssq_out, wbuf, av, wv, ov, lv, rv, ssacc, svr, at, pv, sb, sp, sg,
           al_sem, ap_send, ap_recv, ax_send, ax_recv, ay_send, ay_recv, ao_recv, af_send, af_recv,
           wp_send, wp_recv, wa_send, wa_recv, wf_send, wf_recv, o_send, o_recv,
           wl_sem, r_sem, s_send, s_recv, at_sem, sb_send, sb_recv, sp_send, sp_recv, sf_send, sf_recv):
    rows, cols = r.shape
    last = cols // CN - 1
    quarter = rows // ny
    piece = quarter // PIECES
    tile = min(256, rows)
    me, y = lax.axis_index("tp"), lax.axis_index("tp2")
    x, c = lax.div(me, CORES), lax.rem(me, CORES)
    o = 1 - c
    xa = x + 1 - 2 * lax.rem(x, 2)
    xb = chips - 1 - x
    xab = chips - 1 - xa
    yp, ym = lax.rem(y + 1, ny), lax.rem(y + ny - 1, ny)
    part = {"tp": x * CORES + o}
    acore, aother = {"tp": xa * CORES + c}, {"tp": xa * CORES + o}
    bcore, bother = {"tp": xb * CORES + c}, {"tp": xb * CORES + o}
    up, down = {"tp2": yp}, {"tp2": ym}

    def remote(src, dst, send, recv, device):
        return pltpu.make_async_remote_copy(
            src_ref=src, dst_ref=dst, send_sem=send, recv_sem=recv, device_id=device, device_id_type=MESH)

    def arow(owner, size=None, shift=0):
        return pl.ds(pl.multiple_of(owner * rows + shift, 16), rows if size is None else size)

    def qrow(q, t):
        return pl.ds(pl.multiple_of(q * quarter + t * piece, 16), piece)

    def wcol(j):
        return pl.ds(pl.multiple_of(j * CN, CN), CN)

    own_rows = (xb * CORES + c, me)
    part_rows = (xb * CORES + o, x * CORES + o)

    def a_local(g):
        return pltpu.make_async_copy(a.at[arow(own_rows[g])], av.at[g, 0], al_sem.at[g])

    def a_part(g):
        return remote(a.at[arow(part_rows[g])], av.at[g, 1], ap_send, ap_recv.at[g], part)

    def a_cross(g, s, t):
        core, device = ((c, acore), (o, aother))[s]
        owner = (xab, xa)[g] * CORES + core
        return remote(a.at[arow(owner, piece, y * quarter + t * piece)], av.at[g, 2 + s, qrow(y, t)],
                      ax_send, ax_recv.at[g, s, t], device)

    def a_near(g, s, t, d):
        ref = av.at[g, 2 + s, qrow(y, t)]
        recv = ay_recv.at[g, s, t] if d == s else ao_recv.at[g, max(t - 1, 0)]
        return remote(ref, ref, ay_send, recv, (up, down)[d])

    def a_far(g, s, t):
        ref = av.at[g, 2 + s, qrow((ym, yp)[s], t)]
        return remote(ref, ref, af_send, af_recv.at[g, max(t - 1, 0)], (up, down)[s])

    def a_first(g, s, t):
        a_cross(g, s, t).wait_recv()
        for d in range(2):
            a_near(g, s, t, d).start()

    def a_second(g, s, t):
        a_near(g, s, t, s).wait_recv()
        a_far(g, s, t).start()

    def group_arrival(sem, g, group):
        ref = av.at[g, 2, pl.ds(0, 2 * piece * (2 if group == 0 else 1))]
        return remote(ref, ref, ay_send, sem.at[g, group], part)

    def a_third(g, group):
        group_arrival(ao_recv, g, group).wait_recv()

    def a_fourth(g, group):
        group_arrival(af_recv, g, group).wait_recv()

    def w_part(j):
        return remote(w.at[:, wcol(j)], wbuf.at[0, j], wp_send, wp_recv.at[j], part)

    def w_cross(j):
        return remote(w.at[:, wcol(j)], wbuf.at[1, j], wa_send, wa_recv.at[j], acore)

    def w_pass(j):
        return remote(wbuf.at[1, j], wbuf.at[2, j], wf_send, wf_recv.at[j], part)

    def w_load(g, j, k):
        src = w.at[:, wcol(j)] if k == 0 else wbuf.at[k - 1, j]
        return pltpu.make_async_copy(src, wv.at[g, k], wl_sem.at[g, k])

    def w_loads(g, j):
        for k in range(4):
            w_load(g, j, k).start()

    def out_copy(j):
        slot = lax.rem(j, 2)
        return remote(ov.at[slot], hbuf.at[j], o_send.at[slot], o_recv.at[j], bcore)

    def quarter_of(k):
        return lax.rem(y + lax.div(k + 1, 2) * (2 * lax.rem(k, 2) - 1) + ny, ny)

    def out_rows(i):
        return pl.ds(pl.multiple_of(quarter_of(i) * quarter, 16), quarter)

    def out_part(j, rs):
        slot = lax.rem(j, 2)
        return remote(ov.at[slot, rs], hbuf.at[j, rs], o_send.at[slot], o_recv.at[j], bcore)

    def r_load(j):
        return pltpu.make_async_copy(r.at[:, wcol(j)], rv, r_sem)

    def block_product(lhs, rhs):
        return jnp.dot(lhs, rhs, preferred_element_type=jnp.float32).astype(jnp.bfloat16)

    def summed(g, buf, rs):
        acc = None
        for k in range(4):
            prod = block_product(av[g, k, rs, :], wv[buf, k]).astype(jnp.float32)
            acc = prod if acc is None else acc + prod
        return acc

    def in_parts(j):
        return j <= 8

    def gemm_out(j):
        slot = lax.rem(j, 2)

        def step(i, carry):
            rs = out_rows(i)
            ov[slot, rs, :] = summed(0, 0, rs)

            @pl.when((i >= 1) & in_parts(j))
            def _():
                out_part(j, out_rows(i - 1)).start()

            return carry

        lax.fori_loop(0, ny, step, 0)

    def load_chunk(j, buf):
        with jax.named_scope("w_cross_wait"):
            w_cross(j).wait_recv()
        w_pass(j).start()
        w_load(buf, j, 0).start()
        w_load(buf, j, 2).start()
        with jax.named_scope("w_pass_wait"):
            w_part(j).wait_recv()
            w_load(buf, j, 1).start()
            w_pass(j).wait_recv()
            w_load(buf, j, 3).start()

    def load_wait(j, buf):
        with jax.named_scope("w_load_wait"):
            for k in range(4):
                w_load(buf, j, k).wait()

    most = (PIECES - 1) * ny

    def first_part(n):
        late = lax.div(n, 2 * most)
        early = 1 - late
        j = late * lax.rem(n, 2) + early * lax.div(n, most)
        t = late * (PIECES - 1) + early * lax.div(lax.rem(n, most), ny)
        k = late * lax.div(n - 2 * most, 2) + early * lax.rem(n, ny)
        return j, pl.ds(pl.multiple_of(quarter_of(k) * quarter + t * piece, 16), piece)

    def pass_on(t):
        for s in range(2):
            a_first(0, s, t)
        for s in range(2):
            a_second(0, s, t)
        a_third(0, t - 1)

    def first_chunks():
        def step(n, carry):
            @pl.when(n == ny - 1)
            def _():
                a_fourth(0, 0)

            @pl.when(n == 2 * ny)
            def _():
                with jax.named_scope("a0_piece2"):
                    pass_on(2)

            @pl.when(n == 3 * ny - 1)
            def _():
                with jax.named_scope("a0_far2"):
                    a_fourth(0, 1)

            @pl.when(n == most)
            def _():
                load_chunk(1, 1)
                load_wait(1, 1)

            @pl.when(n == 2 * most)
            def _():
                with jax.named_scope("a0_piece3"):
                    pass_on(3)

            @pl.when(n == 2 * most + 2 * ny - 2)
            def _():
                with jax.named_scope("a0_far3"):
                    a_fourth(0, 2)

            j, rs = first_part(n)
            ov[j, rs, :] = summed(0, j, rs)

            @pl.when(n >= 1)
            def _():
                out_part(*first_part(n - 1)).start()

            return carry

        lax.fori_loop(0, 2 * PIECES * ny, step, 0)
        out_part(*first_part(2 * PIECES * ny - 1)).start()

    def gemm_own(buf):
        def step(i, carry):
            rs = pl.ds(pl.multiple_of(i * tile, tile), tile)
            lv[rs, :] = summed(1, buf, rs)
            return carry

        lax.fori_loop(0, rows // tile, step, 0)

    items = ((xb, 0), (xb, 1), (xab, 0), (xab, 1), (x, o), (xa, o), (x, c), (xa, c))

    def at_load(n):
        pos, core = items[n]
        return pltpu.make_async_copy(a.at[arow(pos * CORES + core)], at.at[n % 2], at_sem.at[n % 2])

    def item_send(n):
        if n < 4:
            slot = n // 2 * 2 + c
            device = {"tp": xb * CORES + n % 2}
            return remote(pv.at[n], sb.at[slot], sb_send, sb_recv.at[slot], device)
        return remote(pv.at[n], sp.at[n - 4], sp_send, sp_recv.at[n - 4], part)

    def item(n):
        at_load(n).wait()

        def step(i, carry):
            rs = pl.ds(pl.multiple_of(i * tile, tile), tile)
            pv[n, rs, :] = block_product(at[n % 2, rs, :], wv[0, 0])
            return carry

        lax.fori_loop(0, rows // tile, step, 0)
        if n + 2 < len(items):
            at_load(n + 2).start()

    def sb_arrival(slot):
        return remote(pv.at[0], sb.at[slot], sb_send, sb_recv.at[slot], bcore)

    def sf_copy():
        return remote(sg, hbuf.at[last], sf_send, sf_recv, acore)

    def for_rows(body):
        def step(t, carry):
            body(pl.ds(pl.multiple_of(t * 64, 64), 64))
            return carry

        lax.fori_loop(0, rows // 64, step, 0)

    def finish(j, rs, h):
        hbuf[j, rs, :] = h
        sq = h * h
        acc = ssacc[rs, :]
        for l in range(CN // 128):
            acc = acc + sq[:, l * 128:(l + 1) * 128]
        ssacc[rs, :] = acc

    def wide(v):
        return v.astype(jnp.float32)

    barrier = pltpu.get_barrier_semaphore()
    peers = [part, acore, aother, bcore, bother] + [{"tp2": lax.rem(y + d, ny)} for d in range(1, ny)]
    for peer in peers:
        pl.semaphore_signal(barrier, inc=1, device_id=peer, device_id_type=MESH)
    w_last = pltpu.make_async_copy(w.at[:, wcol(last)], wv.at[0, 0], wl_sem.at[0, 0])
    w_last.start()
    at_load(0).start()
    at_load(1).start()
    pl.semaphore_wait(barrier, len(peers))

    for t in range(2):
        for s in range(2):
            a_cross(0, s, t).start()
    a_part(0).start()
    for j in range(FIRST):
        w_cross(j).start()
        w_part(j).start()
        if j < 2:
            for s in range(2):
                a_cross(0, s, j + 2).start()
        if j == 4:
            for t in range(PIECES):
                a_cross(1, 0, t).start()
        if j in (6, 7):
            for t in range(2):
                a_cross(1, 1, 2 * (j - 6) + t).start()
    a_part(1).start()
    w_last.wait()
    with jax.named_scope("items"):
        item(0)
        item(1)
        item_send(0).start()
        item(2)
        item_send(1).start()
        item(3)
        item_send(2).start()
    a_local(0).start()
    a_local(1).start()
    ssacc[...] = jnp.zeros_like(ssacc)
    item_send(3).start()
    with jax.named_scope("a0_first"):
        for t in range(2):
            for s in range(2):
                a_first(0, s, t)
    with jax.named_scope("items_2"):
        for n in range(4, 8):
            item(n)
        item_send(4).start()
        item_send(5).start()
    with jax.named_scope("a0_second"):
        for t in range(2):
            for s in range(2):
                a_second(0, s, t)
    with jax.named_scope("a0_third"):
        a_local(0).wait()
        a_part(0).wait_recv()
        a_third(0, 0)
    load_chunk(0, 0)
    load_wait(0, 0)
    with jax.named_scope("first_chunks"):
        first_chunks()

    def merge_last():
        r_load(last).start()
        sb_arrival(0).wait_recv()
        sb_arrival(1).wait_recv()
        with jax.named_scope("sf_wait"):
            sf_copy().wait_recv()
        r_load(last).wait()
        for_rows(lambda rs: finish(last, rs, wide(rv[rs, :]) + (
            (wide(pv[6, rs, :]) + wide(sp[0, rs, :])) + (wide(sb[0, rs, :]) + wide(sb[1, rs, :])) + hbuf[last, rs, :])))

    def sum_last():
        for n in range(2):
            item_send(4 + n).wait_recv()
            sb_arrival(2 + n).wait_recv()

        def body(rs):
            sg[rs, :] = (wide(pv[7, rs, :]) + wide(sp[1, rs, :])) + (wide(sb[2, rs, :]) + wide(sb[3, rs, :]))

        for_rows(body)

    def step(j, carry):
        @pl.when(j < last)
        def _():
            load_chunk(j, 0)

            @pl.when(j + AHEAD < last)
            def _():
                w_cross(j + AHEAD).start()
                w_part(j + AHEAD).start()

            with jax.named_scope("o_send_wait"):
                out_copy(j - 2).wait_send()
            load_wait(j, 0)
            with jax.named_scope("gemm0"):
                gemm_out(j)

            @pl.when(in_parts(j))
            def _():
                out_part(j, out_rows(ny - 1)).start()

            @pl.when(jnp.logical_not(in_parts(j)))
            def _():
                out_copy(j).start()

        @pl.when(j == LAG)
        def _():
            w_loads(1, 1)

        @pl.when((j >= LAG) & (2 * (j - LAG) < last))
        def _():
            w_loads(0, 2 * (j - LAG))

        @pl.when(j == 4)
        def _():
            with jax.named_scope("a1_4"):
                for t in range(PIECES):
                    a_first(1, 0, t)

        @pl.when(j == 5)
        def _():
            with jax.named_scope("a1_5"):
                for t in range(PIECES):
                    a_second(1, 0, t)

        @pl.when(j == LAG - 1)
        def _():
            with jax.named_scope("a1_6"):
                for t in range(2):
                    a_first(1, 1, t)
                for t in range(2):
                    a_second(1, 1, t)

        @pl.when(j == LAG)
        def _():
            with jax.named_scope("a1_7"):
                for t in range(2, PIECES):
                    a_first(1, 1, t)
                for t in range(2, PIECES):
                    a_second(1, 1, t)
                a_local(1).wait()
                a_part(1).wait_recv()
                for group in range(3):
                    a_third(1, group)
                    a_fourth(1, group)

        @pl.when(j == last - 3)
        def _():
            with jax.named_scope("sum_last"):
                sum_last()

        @pl.when(j == last)
        def _():
            with jax.named_scope("drain"):
                drain()

        @pl.when(j == last + 1)
        def _():
            with jax.named_scope("merge_last"):
                merge_last()

        def own(i, inner):
            buf = lax.rem(i, 2)
            r_load(i).start()
            with jax.named_scope("local_load_wait"):
                for k in range(4):
                    w_load(buf, i, k).wait()
            with jax.named_scope("gemm1"):
                gemm_own(buf)

            @pl.when((buf == 1) & (i + 2 < last))
            def _():
                w_loads(1, i + 2)

            r_load(i).wait()
            with jax.named_scope("o_recv_wait"):
                out_copy(i).wait_recv()
            with jax.named_scope("merge"):
                for_rows(lambda rs: finish(i, rs, wide(rv[rs, :]) + (lv[rs, :] + hbuf[i, rs, :])))
            return inner

        @pl.when(j >= LAG)
        def _():
            n = 2 * (j - LAG)
            lax.fori_loop(jnp.maximum(n - 1, 0), jnp.minimum(n + 1, last), own, 0)

        @pl.when(j == last - 3)
        def _():
            sf_copy().start()

        return carry

    def drain():
        def sent(ref, sem):
            remote(ref, ref, sem, sf_recv, part).wait_send()

        sent(wbuf.at[1], wa_send)
        sent(wbuf.at[0], wp_send)
        sent(wbuf.at[2], wf_send)
        sent(av.at[0, pl.ds(0, 2)], ap_send)
        sent(av.at[0, 0], ax_send)
        sent(av.at[0, pl.ds(0, 2)], ay_send)
        sent(av.at[0, 0], af_send)
        sent(sb, sb_send)
        sent(sp, sp_send)

    lax.fori_loop(2, LAG + (last + 1) // 2, step, 0)

    with jax.named_scope("sums"):
        full = lax.dot_general(jnp.ones((8, 128), jnp.float32), ssacc[...], (((1,), (1,)), ((), ())),
                               preferred_element_type=jnp.float32, precision=lax.Precision.HIGHEST)
        line = lax.broadcasted_iota(jnp.int32, (8, 128), 0)
        packed = jnp.zeros((8, 128), jnp.float32)
        for b in range(rows // 128):
            packed = jnp.where(line == b, full[:, b * 128:(b + 1) * 128], packed)
        svr[y] = packed
        sf_copy().wait_send()
        out_copy(last - 2).wait_send()
        out_copy(last - 1).wait_send()
    with jax.named_scope("sums_exchange"):
        sums = [remote(svr.at[y], svr.at[y], s_send, s_recv.at[d - 1], {"tp2": lax.rem(y + d, ny)})
                for d in range(1, ny)]
        for copy in sums:
            copy.start()
        for d in range(1, ny):
            src = lax.rem(y + ny - d, ny)
            remote(svr.at[src], svr.at[src], s_send, s_recv.at[d - 1], part).wait_recv()
        total = svr[0]
        for q in range(1, ny):
            total = total + svr[q]
        ssq_out[...] = total
        ref = svr.at[pl.ds(0, ny - 1)]
        remote(ref, ref, s_send, s_recv.at[0], part).wait_send()


def norm_kernel(width, h, ssq, gain, hidden, normed, scale, hs, ns, h_sem, n_sem):
    chunks, rows, cols = h.shape
    span = 64
    inv_rms = lax.rsqrt(ssq[...] / width + EPS_NORM)
    columns = jnp.transpose(inv_rms)
    for b in range(rows // 128):
        scale[b * 128:(b + 1) * 128, :] = jnp.broadcast_to(columns[:, b:b + 1], (128, scale.shape[1]))

    def block(t, carry):
        rs = pl.ds(pl.multiple_of(t * span, span), span)
        factor = scale[rs, :]
        for j in range(chunks):
            cs = slice(j * cols, (j + 1) * cols)
            value = h[j, rs, :]
            hs[rs, cs] = value.astype(jnp.bfloat16)
            ns[rs, cs] = (value * factor * gain[:, cs]).astype(jnp.bfloat16)
        pltpu.make_async_copy(hs.at[rs], hidden.at[rs], h_sem).start()
        pltpu.make_async_copy(ns.at[rs], normed.at[rs], n_sem).start()
        return carry

    lax.fori_loop(0, rows // span, block, 0)
    pltpu.make_async_copy(hs, hidden, h_sem).wait()
    pltpu.make_async_copy(ns, normed, n_sem).wait()


def solution(mesh):
    tp, ny = mesh.shape["tp"], mesh.shape["tp2"]
    chips = tp // CORES

    def local_step(a, w, r, gain):
        depth, cols = w.shape
        rows = r.shape[0]
        last = cols // CN - 1
        dma = pltpu.SemaphoreType.DMA
        any_space = pl.BlockSpec(memory_space=pl.ANY)
        bf16, f32 = jnp.bfloat16, jnp.float32
        chunks = last + 1
        vmem = pl.BlockSpec(memory_space=pltpu.VMEM)
        h, ssq, _ = pl.pallas_call(
            functools.partial(kernel, ny, chips),
            out_shape=(
                pltpu.VMEM((chunks, rows, CN), f32),
                pltpu.VMEM((8, 128), f32),
                jax.ShapeDtypeStruct((3, last, depth, CN), bf16),
            ),
            in_specs=[any_space] * 3,
            out_specs=(vmem, vmem, any_space),
            scratch_shapes=[
                pltpu.VMEM((2, 4, rows, depth), bf16),
                pltpu.VMEM((2, 4, depth, CN), bf16),
                pltpu.VMEM((2, rows, CN), f32),
                pltpu.VMEM((rows, CN), f32),
                pltpu.VMEM((rows, CN), bf16),
                pltpu.VMEM((rows, 128), f32),
                pltpu.VMEM((ny, 8, 128), f32),
                pltpu.VMEM((2, rows, depth), bf16),
                pltpu.VMEM((8, rows, CN), bf16),
                pltpu.VMEM((4, rows, CN), bf16),
                pltpu.VMEM((2, rows, CN), bf16),
                pltpu.VMEM((rows, CN), f32),
                dma((2,)), dma(()), dma((2,)), dma(()), dma((2, 2, PIECES)),
                dma(()), dma((2, 2, PIECES)), dma((2, 3)), dma(()), dma((2, 3)),
                dma(()), dma((last,)), dma(()), dma((last,)), dma(()), dma((last,)),
                dma((2,)), dma((last,)),
                dma((2, 4)), dma(()), dma(()), dma((ny - 1,)),
                dma((2,)), dma(()), dma((4,)), dma(()), dma((2,)), dma(()), dma(()),
            ],
            compiler_params=pltpu.CompilerParams(
                collective_id=0, has_side_effects=True, vmem_limit_bytes=54400000),
            cost_estimate=pl.CostEstimate(
                flops=2 * 8 * rows * depth * cols, bytes_accessed=8 * depth * cols * 2, transcendentals=0),
        )(a, w, r)
        return pl.pallas_call(
            functools.partial(norm_kernel, cols * ny),
            out_shape=(jax.ShapeDtypeStruct((rows, cols), bf16),) * 2,
            in_specs=[vmem] * 3,
            out_specs=(any_space, any_space),
            scratch_shapes=[
                pltpu.VMEM((rows, CN), f32), pltpu.VMEM((rows, cols), bf16), pltpu.VMEM((rows, cols), bf16),
                dma(()), dma(()),
            ],
            compiler_params=pltpu.CompilerParams(vmem_limit_bytes=24 << 20),
            cost_estimate=pl.CostEstimate(flops=4 * rows * cols, bytes_accessed=8 * rows * cols, transcendentals=rows),
        )(pltpu.with_memory_space_constraint(h, pltpu.VMEM), pltpu.with_memory_space_constraint(ssq, pltpu.VMEM), gain.reshape(1, cols))

    row_spec = P(("dp", "tp"), "tp2")
    return jax.shard_map(local_step, mesh=mesh, in_specs=(P("dp", "tp"), P("tp", "tp2"), row_spec, P("tp2")),
                         out_specs=(row_spec, row_spec), check_vma=False)
```
